128 devices in a mesh: gy: 16 (over z, x), gx: 8 (over y, core).
Axes of the slice: x: 4, y: 4, z: 4, core: 2. Of those that a mesh axis runs over, the one named last changes fastest.
Arguments:
- ensemble: bfloat16 [32, 2, 1024, 1024], P(None, None, 'gy', 'gx'), may hold values from -1.1953125 to 1.1953125
- obs_cell: int32 [16, 8, 2048], P('gy', 'gx'), may hold values from 0 to 8191
- obs_level: int32 [16, 8, 2048], P('gy', 'gx'), may hold values from 0 to 1
- innovation: float32 [16, 8, 2048], P('gy', 'gx'), may hold values from -6 to 6
- obs_weight: float32 [16, 8, 2048], P('gy', 'gx'), may hold values from 0.5 to 4
Outputs:
- control: float32 [32, 2, 1024, 1024], P(None, None, 'gy', 'gx')
- increment: float32 [2, 1024, 1024], P(None, 'gy', 'gx')
The draws below stay inside these ranges and needn't reach their ends.
Inputs may be any that keep to these rules, and one draw needn't show every extreme that they name: obs_cell holds row * 128 + column of the observation within its device's block of 64 x 128 cells.
All inputs are finite; a program needn't handle non-finite values.
Results may differ from the reference program's by a relative error of at most 0.0003.
Values sent between devices are 32-bit elements; how exact they have to be, the bound alone decides.
A program may use at most 128 MiB of HBM per device.

```python
import math
import jax
import jax.numpy as jnp
from jax import lax

MEMBERS = 32
LEV = 2
SWEEPS = 4
CY = 64
CX = 128
OBS_DEV = 2048
NY = 1024
NX = 1024
N_GY = 16
N_GX = 8


def place_ends(result, key, smallest, high):
    dims = result.shape
    place = [jax.random.randint(jax.random.fold_in(key, axis), (), 0, dims[axis]) for axis in range(len(dims))]
    result = result.at[tuple(place)].set(smallest)
    longest = dims.index(max(dims))
    place[longest] = (place[longest] + 1) % dims[longest]
    return result.at[tuple(place)].set(high)


def block_scale(stream_key, dims, split, low, top_value):
    level = 1.0
    for axis_at, parts in split:
        draws = jax.random.uniform(jax.random.fold_in(jax.random.fold_in(stream_key, 6), axis_at), (parts,), jnp.float32, low / len(split), top_value / len(split))
        level = level * jnp.repeat(jnp.exp(draws), dims[axis_at] // parts).reshape((-1,) + (1,) * (len(dims) - 1 - axis_at))
    return level


def centred(stream_key, shape, scale, reach, cuts=(), kind=jnp.bfloat16):
    entries = scale * jax.random.normal(stream_key, shape, jnp.float32)
    if cuts:
        entries = entries * block_scale(stream_key, shape, cuts, -0.22, 0.18)
    return jnp.clip(entries, -reach, reach).astype(kind)


def setup_inputs(seed: int = 0) -> dict:
    keys = jax.random.split(jax.random.key(seed), 6)
    return {
        "ensemble": centred(keys[0], (MEMBERS, LEV, NY, NX), 0.2, 1.1953125, ((2, 16), (3, 8))),
        "obs_cell": place_ends(jax.random.randint(keys[1], (N_GY, N_GX, OBS_DEV), 0, CY * CX), jax.random.fold_in(keys[1], 1), 0, (CY * CX) - 1).astype(jnp.int32),
        "obs_level": place_ends(jax.random.randint(keys[2], (N_GY, N_GX, OBS_DEV), 0, LEV), jax.random.fold_in(keys[2], 1), 0, LEV - 1).astype(jnp.int32),
        "innovation": centred(keys[3], (N_GY, N_GX, OBS_DEV), 1.0, 6.0, ((0, 16), (1, 8)), jnp.float32),
        "obs_weight": jnp.clip(jnp.exp(math.log(4.0) - 2.0794415 * jax.random.uniform(keys[4], (N_GY, N_GX, OBS_DEV), jnp.float32) ** block_scale(keys[4], (N_GY, N_GX, OBS_DEV), ((0, 16), (1, 8)), -0.2, 0.2)), 0.5, 4.0),
    }


KAPPA = 0.2
EPS = 1e-06

def smooth_once(field):
    padded = jnp.pad(field, ((0, 0), (0, 0), (1, 1), (1, 1)))
    beside_all = padded[:, :, 2:, 1:-1] + padded[:, :, :-2, 1:-1] + padded[:, :, 1:-1, 2:] + padded[:, :, 1:-1, :-2]
    return field + KAPPA * (beside_all - 4.0 * field)

def filtered(field):
    for sweep in range(SWEEPS):
        field = smooth_once(field)
    return field

def reference(ensemble, obs_cell, obs_level, innovation, obs_weight):
    block_row = jnp.arange(N_GY, dtype=jnp.int32)[:, None, None]
    block_col = jnp.arange(N_GX, dtype=jnp.int32)[None, :, None]
    rows = block_row * CY + obs_cell // CX
    cols = block_col * CX + obs_cell % CX
    points = (obs_level * (NY * NX) + rows * NX + cols).reshape(-1).astype(jnp.int32)
    weights = obs_weight.reshape(-1)
    members = ensemble.astype(jnp.float32)

    def adjoint_obs(values):
        state = jnp.zeros((LEV * NY * NX,), jnp.float32).at[points].add(values)
        return state.reshape(LEV, NY, NX)

    def hessian(vector):
        state = lax.optimization_barrier(jnp.sum(members * filtered(vector), axis=0))
        seen = state.reshape(-1)[points]
        back = filtered(members * adjoint_obs(weights * seen)[None])
        return (vector + back, state)
    gradient = filtered(members * adjoint_obs(weights * innovation.reshape(-1))[None])
    bnorm = jnp.sqrt(jnp.sum(gradient * gradient) + EPS)
    first = gradient / bnorm
    image_one, state_one = hessian(first)
    alpha_one = jnp.sum(first * image_one)
    remain = image_one - alpha_one * first
    beta = jnp.sqrt(jnp.sum(remain * remain) + EPS)
    second = remain / beta
    image_two, state_two = hessian(second)
    alpha_two = jnp.sum(second * image_two)
    determ = alpha_one * alpha_two - beta * beta
    coef_one = bnorm * alpha_two / determ
    coef_two = -bnorm * beta / determ
    control = coef_one * first + coef_two * second
    increment = coef_one * state_one + coef_two * state_two
    return (control, increment)
```

```python
import jax
import jax.numpy as jnp
from jax import lax
from jax.sharding import PartitionSpec as P

SWEEPS = 4
WIDE = 2 * SWEEPS
KAPPA = 0.2
EPS = 1e-06
AXES = ("gy", "gx")


def with_halo(cells, width):
    for axis, dim in (("gy", cells.ndim - 2), ("gx", cells.ndim - 1)):
        count = lax.axis_size(axis)
        ends = count - 1
        head = lax.slice_in_dim(cells, 0, width, axis=dim)
        tail = lax.slice_in_dim(cells, cells.shape[dim] - width, cells.shape[dim], axis=dim)
        cells = jnp.concatenate(
            [
                lax.ppermute(tail, axis, [(i, i + 1) for i in range(ends)]),
                cells,
                lax.ppermute(head, axis, [(i + 1, i) for i in range(ends)]),
            ],
            axis=dim,
        )
    return cells


def four_sweeps(field, depth, rows, cols):
    row_pos = lax.axis_index("gy") * rows - depth + jnp.arange(rows + 2 * depth, dtype=jnp.int32)
    col_pos = lax.axis_index("gx") * cols - depth + jnp.arange(cols + 2 * depth, dtype=jnp.int32)
    row_mask = ((row_pos >= 0) & (row_pos < rows * lax.axis_size("gy"))).astype(jnp.float32)
    col_mask = ((col_pos >= 0) & (col_pos < cols * lax.axis_size("gx"))).astype(jnp.float32)
    mask = KAPPA * row_mask[:, None] * col_mask[None, :]
    for sweep in range(1, SWEEPS + 1):
        total = (
            field[..., 1:-1, 1:-1]
            + (field[..., 2:, 1:-1] + field[..., :-2, 1:-1])
            + (field[..., 1:-1, 2:] + field[..., 1:-1, :-2])
        )
        field = total * mask[sweep : rows + 2 * depth - sweep, sweep : cols + 2 * depth - sweep]
    return field


def on_device(ensemble, obs_cell, obs_level, innovation, obs_weight):
    levels, rows, cols = ensemble.shape[1:]
    points = (obs_level * (rows * cols) + obs_cell).reshape(-1)
    weights = obs_weight.reshape(-1)
    pair = jnp.stack([weights * innovation.reshape(-1), weights], axis=1)
    pair = jnp.zeros((levels * rows * cols, 2), jnp.float32).at[points].add(pair)
    gradient = pair[:, 0].reshape(levels, rows, cols)
    diagonal = pair[:, 1].reshape(levels, rows, cols)
    wide = with_halo(ensemble.astype(jnp.float32), WIDE)

    def image(state):
        field = four_sweeps(wide * with_halo(state, WIDE), WIDE, rows, cols)
        back = jnp.sum(ensemble * four_sweeps(field, SWEEPS, rows, cols), axis=0)
        return field[..., SWEEPS:-SWEEPS, SWEEPS:-SWEEPS], back

    base, base_state = image(gradient)
    seen = diagonal * base_state
    grown, grown_state = image(seen)
    sums = jnp.stack(
        [
            jnp.sum(base * base),
            jnp.sum(seen * base_state),
            jnp.sum(grown * grown),
            jnp.sum(diagonal * grown_state * grown_state),
        ]
    )
    sums = lax.psum(sums, AXES)
    bnorm_sq = sums[0] + EPS
    bnorm = jnp.sqrt(bnorm_sq)
    unit, cross, square, cube = [sums[i] / bnorm_sq for i in range(4)]
    alpha_one = unit + cross
    shift = 1.0 - alpha_one
    remain_sq = jnp.maximum(shift * shift * unit + 2.0 * shift * cross + square, 0.0)
    beta_sq = remain_sq + EPS
    beta = jnp.sqrt(beta_sq)
    curve = jnp.maximum(shift * shift * cross + 2.0 * shift * square + cube, 0.0)
    alpha_two = (remain_sq + curve) / beta_sq
    determ = alpha_one * alpha_two - beta_sq
    coef_one = bnorm * alpha_two / determ
    coef_two = -bnorm * beta / determ
    on_base = coef_one / bnorm + coef_two * shift / (bnorm * beta)
    on_grown = coef_two / (bnorm * beta)
    control = on_base * base + on_grown * grown
    increment = on_base * base_state + on_grown * grown_state
    return (control, increment)


def solution(mesh):
    return jax.shard_map(
        on_device,
        mesh=mesh,
        in_specs=(P(None, None, "gy", "gx"),) + (P("gy", "gx", None),) * 4,
        out_specs=(P(None, None, "gy", "gx"), P(None, "gy", "gx")),
        check_vma=False,
    )
```

```python
import jax
import jax.numpy as jnp
from jax import lax
from jax.experimental import pallas as pl
from jax.experimental.pallas import tpu as pltpu
from jax.sharding import PartitionSpec as P

MESH = pl.DeviceIdType.MESH
F32 = jnp.float32
BF16 = jnp.bfloat16
EPS = 1e-06
FILTER_SCALE = 0.2**4
MEMBERS = 32
LEVELS = 2
ROWS = 64
COLS = 128
HALO = 8
EXT = ROWS + 2 * HALO
STEP = EXT // 8
CHUNKS = 4
PER = 16
OBS_STEP = 512

WAYS = ((-1, 0), (1, 0), (0, -1), (0, 1), (-1, -1), (-1, 1), (1, -1), (1, 1))


def lane_iota():
    return lax.broadcasted_iota(jnp.int32, (8, 128), 1)


def strided(ref, *lead):
    return [ref[(*lead, pl.ds(t, 8, stride=STEP), slice(None))] for t in range(STEP)]


def put_strided(ref, values, *lead):
    for t in range(STEP):
        ref[(*lead, pl.ds(t, 8, stride=STEP), slice(None))] = values[t]


def plus(f):
    out = []
    for t in range(STEP):
        up = f[t - 1] if t else pltpu.roll(f[STEP - 1], 1, 0)
        down = f[t + 1] if t < STEP - 1 else pltpu.roll(f[0], 7, 0)
        side = pltpu.roll(f[t], 1, 1) + pltpu.roll(f[t], 127, 1)
        out.append((f[t] + (up + down)) + side)
    return out


def total(values):
    while len(values) > 1:
        odd = values[len(values) - len(values) % 2 :]
        values = [a + b for a, b in zip(values[0::2], values[1::2])] + odd
    return values[0]


def kernel(
    n_gy,
    n_gx,
    ens,
    cell,
    level,
    innov,
    weight,
    control,
    increment,
    xin,
    cin,
    lin,
    iin,
    win,
    ext,
    xpk,
    xst,
    sext,
    spk,
    sst,
    dext,
    grid,
    xpm,
    xpr,
    fm,
    fr,
    piece_m,
    piece_r,
    acc_m,
    acc_r,
    sq_m,
    sq_r,
    image,
    rowa,
    rowb,
    staged,
    sinc,
    in_sem,
    xsend,
    xrecv,
    ssend,
    srecv,
    asend,
    arecv,
    bsend,
    brecv,
    out_sem,
):
    gy = lax.axis_index("gy")
    gx = lax.axis_index("gx")
    lane = lane_iota()
    sub = lax.broadcasted_iota(jnp.int32, (8, 128), 0)

    loads = [
        pltpu.make_async_copy(src, dst, in_sem.at[i])
        for i, (src, dst) in enumerate(((ens, xin), (cell, cin), (level, lin), (innov, iin), (weight, win)))
    ]
    for load in loads:
        load.start()

    def there(dy, dx):
        return (lax.rem(gy + dy + n_gy, n_gy), lax.rem(gx + dx + n_gx, n_gx))

    barrier = pltpu.get_barrier_semaphore()
    met = [(0, k) for k in range(1, n_gx)] + [(k, 0) for k in range(1, n_gy)] + list(WAYS[4:])
    for dy, dx in met:
        pl.semaphore_signal(barrier, inc=1, device_id=there(dy, dx), device_id_type=MESH)

    loads[0].wait()

    def widen(c, carry):
        east = [jnp.zeros((8, 128), F32)] * 8
        west = [jnp.zeros((8, 128), F32)] * 8
        for lev in range(LEVELS):
            for mm in range(8):
                j = lev * 8 + mm
                x = xin[c * 8 + mm, lev].astype(F32)
                ext[c * PER + j, HALO : HALO + ROWS, :] = x
                here = (lane >= 8 * j) & (lane < 8 * j + 8)
                for k in range(8):
                    part = x[8 * k : 8 * k + 8]
                    turned = pltpu.roll(part, 8 * j, 1) if j else part
                    west[k] = jnp.where(here, turned, west[k])
                    turned = pltpu.roll(part, (8 * j + 8) % 128, 1) if (8 * j + 8) % 128 else part
                    east[k] = jnp.where(here, turned, east[k])
        for k in range(8):
            xpk[0, c, 8 * k : 8 * k + 8, :] = west[k]
            xpk[1, c, 8 * k : 8 * k + 8, :] = east[k]
        return carry

    lax.fori_loop(0, CHUNKS, widen, 0)

    def messages(wide, west, east, from_west, from_east, send, recv):
        top, low = pl.ds(HALO, HALO), pl.ds(ROWS, HALO)
        pairs = (
            (wide.at[:, top, :], wide.at[:, pl.ds(HALO + ROWS, HALO), :]),
            (wide.at[:, low, :], wide.at[:, pl.ds(0, HALO), :]),
            (west, from_east.at[pl.ds(HALO, ROWS), :]),
            (east, from_west.at[pl.ds(HALO, ROWS), :]),
            (west.at[pl.ds(0, HALO), :], from_east.at[pl.ds(HALO + ROWS, HALO), :]),
            (east.at[pl.ds(0, HALO), :], from_west.at[pl.ds(HALO + ROWS, HALO), :]),
            (west.at[pl.ds(ROWS - HALO, HALO), :], from_east.at[pl.ds(0, HALO), :]),
            (east.at[pl.ds(ROWS - HALO, HALO), :], from_west.at[pl.ds(0, HALO), :]),
        )
        return [
            pltpu.make_async_remote_copy(
                src_ref=src,
                dst_ref=dst,
                send_sem=send.at[way],
                recv_sem=recv.at[way],
                device_id=there(*WAYS[way]),
                device_id_type=MESH,
            )
            for way, (src, dst) in enumerate(pairs)
        ]

    pl.semaphore_wait(barrier, len(met))
    sent = []
    xmsgs = []
    for c in range(CHUNKS):
        msgs = messages(
            ext.at[pl.ds(c * PER, PER)],
            xpk.at[0, c],
            xpk.at[1, c],
            xst.at[0, c],
            xst.at[1, c],
            xsend.at[c],
            xrecv.at[c],
        )
        for msg in msgs:
            msg.start()
        xmsgs.append(msgs)
        sent += msgs

    for load in loads[1:]:
        load.wait()
    grid[...] = jnp.zeros_like(grid)

    def scatter(k, carry):
        part = pl.ds(pl.multiple_of(k * OBS_STEP, OBS_STEP), OBS_STEP)
        where_at = cin[0, :, part]
        row = where_at >> 7
        col = (where_at & 127) + lin[0, :, part] * COLS
        w = win[0, :, part]
        on_row = lax.broadcasted_iota(jnp.int32, (ROWS, OBS_STEP), 0) == row
        on_col = lax.broadcasted_iota(jnp.int32, (LEVELS * COLS, OBS_STEP), 0) == col
        right = jnp.where(on_col, 1.0, 0.0).astype(BF16)
        left = []
        for value in (w * iin[0, :, part], w):
            for _ in range(3):
                piece = value.astype(BF16).astype(F32)
                left.append(jnp.where(on_row, piece, 0.0).astype(BF16))
                value = value - piece
        left = jnp.concatenate(left, axis=0)
        grid[...] += lax.dot_general(left, right, (((1,), (1,)), ((), ())), preferred_element_type=F32)
        return carry

    lax.fori_loop(0, cin.shape[-1] // OBS_STEP, scatter, 0)
    for lev in range(LEVELS):
        cols = slice(lev * COLS, lev * COLS + COLS)
        grad = grid[0:64, cols] + (grid[64:128, cols] + grid[128:192, cols])
        diag = grid[192:256, cols] + (grid[256:320, cols] + grid[320:384, cols])
        sext[0, lev, HALO : HALO + ROWS, :] = grad
        dext[lev, 0:HALO, :] = jnp.zeros((HALO, COLS), F32)
        dext[lev, HALO : HALO + ROWS, :] = diag
        dext[lev, HALO + ROWS : EXT, :] = jnp.zeros((HALO, COLS), F32)

    def share_state(kind):
        for k in range(8):
            at = HALO + 8 * k
            a = sext[kind, 0, at : at + 8, :]
            b = sext[kind, 1, at : at + 8, :]
            spk[kind, 0, 8 * k : 8 * k + 8, :] = jnp.where(lane < 8, a, pltpu.roll(b, 8, 1))
            spk[kind, 1, 8 * k : 8 * k + 8, :] = jnp.where(lane < 8, pltpu.roll(a, 8, 1), pltpu.roll(b, 16, 1))
        msgs = messages(
            sext.at[kind],
            spk.at[kind, 0],
            spk.at[kind, 1],
            sst.at[kind, 0],
            sst.at[kind, 1],
            ssend.at[kind],
            srecv.at[kind],
        )
        for msg in msgs:
            msg.start()
        return msgs

    def turned_round(x):
        for width in (1, 2, 4):
            low = (lane & width) == 0
            x = jnp.where(low, pltpu.roll(x, 128 - width, 1), pltpu.roll(x, width, 1))
        return x

    def mirror(side, read, strips, sign):
        for k in range(EXT // 8):
            x = turned_round(read(k))
            x = pltpu.roll(x, 127, 1) if side == 0 else pltpu.roll(x, 1, 1)
            if sign is not None:
                outside = (lane & 7) == (7 if side == 0 else 0)
                x = jnp.where(outside, 0.0, sign * x)
            strips[8 * k : 8 * k + 8, :] = x

    def mirror_ensemble(c, side):
        def read(k):
            if 1 <= k <= 8:
                return xpk[side, c, 8 * (k - 1) : 8 * k, :]
            out = jnp.zeros((8, 128), F32)
            for j in range(PER):
                part = ext[c * PER + j, 8 * k : 8 * k + 8, :]
                turn = (8 * j + (8 if side else 0)) % 128
                turned = pltpu.roll(part, turn, 1) if turn else part
                out = jnp.where((lane >= 8 * j) & (lane < 8 * j + 8), turned, out)
            return out

        mirror(side, read, xst.at[side, c], None)

    def mirror_state(kind, side):
        def read(k):
            a = sext[kind, 0, 8 * k : 8 * k + 8, :]
            b = sext[kind, 1, 8 * k : 8 * k + 8, :]
            if side == 0:
                return jnp.where(lane < 8, a, pltpu.roll(b, 8, 1))
            return jnp.where(lane < 8, pltpu.roll(a, 8, 1), pltpu.roll(b, 16, 1))

        mirror(side, read, sst.at[kind, side], -1.0)

    keep_north = jnp.where((gy == 0) & (sub == 0), 0.0, 1.0)
    keep_south = jnp.where((gy == n_gy - 1) & (sub == 7), 0.0, 1.0)

    def edged(f):
        f = list(f)
        f[7] = f[7] * keep_north
        f[2] = f[2] * keep_south
        return f

    def filtered(f):
        for _ in range(4):
            f = edged(plus(f))
        return f

    def state_pieces(kind):
        @pl.when(gx == 0)
        def _():
            mirror_state(kind, 0)

        @pl.when(gx == n_gx - 1)
        def _():
            mirror_state(kind, 1)

        west = strided(sst, kind, 0)
        east = strided(sst, kind, 1)
        for lev in range(LEVELS):
            s = strided(sext, kind, lev)
            main = []
            rest = []
            for t in range(STEP):
                w = pltpu.roll(west[t], 120, 1) if lev else west[t]
                main.append(jnp.where(lane < 8, w, pltpu.roll(s[t], 8, 1)) * FILTER_SCALE)
                r = jnp.where(lane < 24, pltpu.roll(s[t], 24, 1), pltpu.roll(east[t], 24 - 8 * lev, 1))
                r = jnp.where(lane < 32, r * FILTER_SCALE, 0.0)
                r = r + pltpu.roll(r, 32, 1)
                rest.append(r + pltpu.roll(r, 64, 1))
            main, rest = edged(main), edged(rest)
            for t in range(STEP):
                piece_m[lev, 8 * t : 8 * t + 8, :] = main[t]
                piece_r[lev, 8 * t : 8 * t + 8, :] = rest[t]

    def tiles(ref, *lead):
        return [ref[(*lead, slice(8 * t, 8 * t + 8), slice(None))] for t in range(STEP)]

    def put_tiles(ref, values, *lead):
        for t in range(STEP):
            ref[(*lead, slice(8 * t, 8 * t + 8), slice(None))] = values[t]

    def add_tiles(ref, values, *lead):
        for t in range(STEP):
            ref[(*lead, slice(8 * t, 8 * t + 8), slice(None))] += values[t]

    def build(c, lev, quad):
        first = c * PER + lev * 8 + quad * 4
        east = strided(xst, 1, c)
        west = strided(xst, 0, c)
        rest = [None] * STEP
        for i in range(4):
            slot = lev * 8 + quad * 4 + i
            x = strided(ext, first + i)
            back = lax.rem(256 - 8 * slot, 128)
            fore = lax.rem(256 + 32 * i + 24 - 8 * slot, 128)
            main = []
            for t in range(STEP):
                main.append(jnp.where(lane < 8, pltpu.roll(west[t], back, 1), pltpu.roll(x[t], 8, 1)))
                turned = pltpu.roll(x[t], (32 * i + 24) % 128, 1)
                part = jnp.where(lane < 32 * i + 24, turned, pltpu.roll(east[t], fore, 1))
                rest[t] = part if i == 0 else jnp.where(lane < 32 * i, rest[t], part)
            put_tiles(xpm, main, first + i)
        put_tiles(xpr, rest, c * 4 + lev * 2 + quad)

    def apply_piece(kind, x, xi, s, f_ref, fi):
        f = filtered([a * b for a, b in zip(tiles(x, xi), s)])
        put_tiles(f_ref, f, kind, fi)
        square = [a * a for a in f]
        f = filtered(f)
        return square, [a * b for a, b in zip(f, tiles(x, xi))]

    def apply(kind, index, carry):
        c = index // 4
        lev = lax.rem(index // 2, 2)
        quad = lax.rem(index, 2)
        first = c * PER + lev * 8 + quad * 4
        s = tiles(piece_m, lev)
        squares, images = None, None
        for i in range(4):
            square, out = apply_piece(kind, xpm, first + i, s, fm, first + i)
            squares = square if i == 0 else [a + b for a, b in zip(squares, square)]
            images = out if i == 0 else [a + b for a, b in zip(images, out)]
        add_tiles(acc_m, images, lev)
        add_tiles(sq_m, squares, kind)
        square, out = apply_piece(kind, xpr, index, tiles(piece_r, lev), fr, index)
        add_tiles(acc_r, out, lev)
        add_tiles(sq_r, square, kind)
        return carry

    def state_image(kind):
        for lev in range(LEVELS):
            main = tiles(acc_m, lev)
            rest = tiles(acc_r, lev)
            out = []
            for t in range(STEP):
                r = rest[t] + pltpu.roll(rest[t], 64, 1)
                r = r + pltpu.roll(r, 32, 1)
                out.append(jnp.where(lane < 112, pltpu.roll(main[t], 120, 1), pltpu.roll(r, 104, 1)) * FILTER_SCALE)
            put_tiles(image, out, kind, lev)

    def clear():
        acc_m[...] = jnp.zeros_like(acc_m)
        acc_r[...] = jnp.zeros_like(acc_r)

    sq_m[...] = jnp.zeros_like(sq_m)
    sq_r[...] = jnp.zeros_like(sq_r)
    clear()
    smsgs = share_state(0)
    sent += smsgs
    for msg in smsgs:
        msg.wait_recv()
    state_pieces(0)
    for c in range(CHUNKS):
        for msg in xmsgs[c]:
            msg.wait_recv()

        @pl.when(gx == 0)
        def _():
            mirror_ensemble(c, 0)

        @pl.when(gx == n_gx - 1)
        def _():
            mirror_ensemble(c, 1)

        def first_pass(index, carry):
            build(index // 4, lax.rem(index // 2, 2), lax.rem(index, 2))
            return apply(0, index, carry)

        lax.fori_loop(4 * c, 4 * c + 4, first_pass, 0)
    state_image(0)

    for lev in range(LEVELS):
        v = [a * b for a, b in zip(tiles(image, 0, lev), strided(dext, lev))]
        put_strided(staged, v, lev)
        sext[1, lev, HALO : HALO + ROWS, :] = staged[lev, HALO : HALO + ROWS, :]
    smsgs = share_state(1)
    sent += smsgs
    clear()
    for msg in smsgs:
        msg.wait_recv()
    state_pieces(1)
    lax.fori_loop(0, CHUNKS * 4, lambda i, carry: apply(1, i, carry), 0)
    state_image(1)

    def norm(kind):
        rest_lane = lane & 31
        parts = []
        for t in range(STEP):
            row = sub * STEP + t
            inside = (row >= HALO) & (row < HALO + ROWS)
            main_in = inside & (lane >= 8) & (lane < 120)
            rest_in = inside & (rest_lane >= 8) & (rest_lane < 24)
            parts.append(jnp.where(main_in, sq_m[kind, 8 * t : 8 * t + 8, :], 0.0))
            parts.append(jnp.where(rest_in, sq_r[kind, 8 * t : 8 * t + 8, :], 0.0))
        return jnp.sum(total(parts))

    def weighted(kind):
        parts = []
        for lev in range(LEVELS):
            d = strided(dext, lev)
            x = tiles(image, kind, lev)
            parts += [b * (a * a) for a, b in zip(x, d)]
        return jnp.sum(total(parts))

    mine = (norm(0), weighted(0), norm(1), weighted(1))
    line = lane[0:1]
    row = jnp.where(line < 64, jnp.where(line < 32, mine[0], mine[1]), jnp.where(line < 96, mine[2], mine[3]))

    def gather(value, ref, me, n, send, recv, to):
        ref[me] = value
        copies = []
        for k in range(1, n):
            copies.append(
                pltpu.make_async_remote_copy(
                    src_ref=ref.at[me],
                    dst_ref=ref.at[me],
                    send_sem=send.at[k],
                    recv_sem=recv.at[k],
                    device_id=to(k),
                    device_id_type=MESH,
                )
            )
            copies[-1].start()
        for copy in copies:
            copy.wait_recv()
        return copies, jnp.sum(ref[...], axis=0)

    copies, row = gather(row, rowa, gx, n_gx, asend, arecv, lambda k: there(0, k))
    sent += copies
    copies, row = gather(row, rowb, gy, n_gy, bsend, brecv, lambda k: there(k, 0))
    sent += copies

    sums = [jnp.full((8, 128), jnp.sum(jnp.where(line == 32 * i, row, 0.0)), F32) for i in range(4)]
    bnorm_sq = sums[0] + EPS
    bnorm = jnp.sqrt(bnorm_sq)
    unit, cross, square, cube = [s / bnorm_sq for s in sums]
    alpha_one = unit + cross
    shift = 1.0 - alpha_one
    remain_sq = jnp.maximum(shift * shift * unit + 2.0 * shift * cross + square, 0.0)
    beta_sq = remain_sq + EPS
    beta = jnp.sqrt(beta_sq)
    curve = jnp.maximum(shift * shift * cross + 2.0 * shift * square + cube, 0.0)
    alpha_two = (remain_sq + curve) / beta_sq
    determ = alpha_one * alpha_two - beta_sq
    coef_one = bnorm * alpha_two / determ
    coef_two = -bnorm * beta / determ
    on_base = coef_one / bnorm + coef_two * shift / (bnorm * beta)
    on_grown = coef_two / (bnorm * beta)

    outs = []
    for lev in range(LEVELS):
        x, z = tiles(image, 0, lev), tiles(image, 1, lev)
        put_strided(sinc, [on_base * a + on_grown * b for a, b in zip(x, z)], lev)
    outs.append(pltpu.make_async_copy(sinc.at[:, pl.ds(HALO, ROWS), :], increment, out_sem.at[0]))
    outs[-1].start()

    def finish(index, carry):
        first = (index // 4) * PER + lax.rem(index, 4) * 4
        rest = [on_base * a + on_grown * b for a, b in zip(tiles(fr, 0, index), tiles(fr, 1, index))]
        for i in range(4):
            out = []
            for t, (a, b) in enumerate(zip(tiles(fm, 0, first + i), tiles(fm, 1, first + i))):
                main = pltpu.roll(on_base * a + on_grown * b, 120, 1)
                turn = (104 - 32 * i) % 128
                out.append(jnp.where(lane < 112, main, pltpu.roll(rest[t], turn, 1)))
            put_strided(staged, out, first + i)
        return carry

    for c in range(CHUNKS):
        lax.fori_loop(4 * c, 4 * c + 4, finish, 0)
        for lev in range(LEVELS):
            outs.append(
                pltpu.make_async_copy(
                    staged.at[pl.ds(c * PER + lev * 8, 8), pl.ds(HALO, ROWS), :],
                    control.at[pl.ds(c * 8, 8), lev],
                    out_sem.at[1 + 2 * c + lev],
                )
            )
            outs[-1].start()
    for out in outs:
        out.wait()
    for msg in sent:
        msg.wait_send()


def solution(mesh):
    n_gy, n_gx = mesh.shape["gy"], mesh.shape["gx"]

    def on_device(ensemble, obs_cell, obs_level, innovation, obs_weight):
        obs = obs_cell.shape[-1]
        fields = MEMBERS * LEVELS
        vmem = pltpu.VMEM
        dma = pltpu.SemaphoreType.DMA
        return pl.pallas_call(
            lambda *refs: kernel(n_gy, n_gx, *refs),
            name="lanczos",
            out_shape=(
                jax.ShapeDtypeStruct((MEMBERS, LEVELS, ROWS, COLS), F32),
                jax.ShapeDtypeStruct((LEVELS, ROWS, COLS), F32),
            ),
            in_specs=[pl.BlockSpec(memory_space=pl.ANY)] * 5,
            out_specs=(pl.BlockSpec(memory_space=pl.ANY),) * 2,
            scratch_shapes=[
                vmem((MEMBERS, LEVELS, ROWS, COLS), BF16),
                vmem((1, 1, obs), jnp.int32),
                vmem((1, 1, obs), jnp.int32),
                vmem((1, 1, obs), F32),
                vmem((1, 1, obs), F32),
                vmem((fields, EXT, COLS), F32),
                vmem((2, CHUNKS, ROWS, COLS), F32),
                vmem((2, CHUNKS, EXT, COLS), F32),
                vmem((2, LEVELS, EXT, COLS), F32),
                vmem((2, 2, ROWS, COLS), F32),
                vmem((2, 2, EXT, COLS), F32),
                vmem((LEVELS, EXT, COLS), F32),
                vmem((6 * ROWS, LEVELS * COLS), F32),
                vmem((fields, EXT, COLS), F32),
                vmem((fields // 4, EXT, COLS), F32),
                vmem((2, fields, EXT, COLS), F32),
                vmem((2, fields // 4, EXT, COLS), F32),
                vmem((LEVELS, EXT, COLS), F32),
                vmem((LEVELS, EXT, COLS), F32),
                vmem((LEVELS, EXT, COLS), F32),
                vmem((LEVELS, EXT, COLS), F32),
                vmem((2, EXT, COLS), F32),
                vmem((2, EXT, COLS), F32),
                vmem((2, LEVELS, EXT, COLS), F32),
                vmem((n_gx, 1, COLS), F32),
                vmem((n_gy, 1, COLS), F32),
                vmem((fields, EXT, COLS), F32),
                vmem((LEVELS, EXT, COLS), F32),
                dma((5,)),
                dma((CHUNKS, 8)),
                dma((CHUNKS, 8)),
                dma((2, 8)),
                dma((2, 8)),
                dma((n_gx,)),
                dma((n_gx,)),
                dma((n_gy,)),
                dma((n_gy,)),
                dma((9,)),
            ],
            compiler_params=pltpu.CompilerParams(
                collective_id=0, has_side_effects=True, vmem_limit_bytes=60 * 1024 * 1024
            ),
        )(ensemble, obs_cell, obs_level, innovation, obs_weight)

    return jax.shard_map(
        on_device,
        mesh=mesh,
        in_specs=(P(None, None, "gy", "gx"),) + (P("gy", "gx", None),) * 4,
        out_specs=(P(None, None, "gy", "gx"), P(None, "gy", "gx")),
        check_vma=False,
    )
```

```python
import jax
import jax.numpy as jnp
from jax import lax
from jax.experimental import pallas as pl
from jax.experimental.pallas import tpu as pltpu
from jax.sharding import PartitionSpec as P

MESH = pl.DeviceIdType.MESH
F32 = jnp.float32
BF16 = jnp.bfloat16
EPS = 1e-06
FILTER_SCALE = 0.2**4
MEMBERS = 32
LEVELS = 2
ROWS = 64
COLS = 128
HALO = 8
EROWS = ROWS + 2 * HALO
ECOLS = COLS + 2 * HALO
NR = EROWS // 8
NT = ECOLS // 8
CHUNKS = 4
PER = 16
OBS_STEP = 512

WAYS = ((-1, 0), (1, 0), (0, -1), (0, 1), (-1, -1), (-1, 1), (1, -1), (1, 1))


def total(values):
    while len(values) > 1:
        odd = values[len(values) - len(values) % 2 :]
        values = [a + b for a, b in zip(values[0::2], values[1::2])] + odd
    return values[0]


def by_rows(ref, *lead):
    return [ref[(*lead, pl.ds(r, 8, stride=NR), slice(None))] for r in range(NR)]


def put_rows(ref, values, *lead):
    for r in range(NR):
        ref[(*lead, pl.ds(r, 8, stride=NR), slice(None))] = values[r]


def tiles(ref, *lead):
    return [ref[(*lead, slice(8 * r, 8 * r + 8), slice(None))] for r in range(NR)]


def put_tiles(ref, values, *lead):
    for r in range(NR):
        ref[(*lead, slice(8 * r, 8 * r + 8), slice(None))] = values[r]


def sweep(load, store, masks):
    north, south, west, east = masks
    for first, last in ((0, NT // 2), (NT // 2, NT)):
        seen = {}

        def f(r, t):
            if (r, t) not in seen:
                if t == -1:
                    value = pltpu.roll(f(r, NT - 1), 1, 0)
                elif t == NT:
                    value = pltpu.roll(f(r, 0), 7, 0)
                elif r == -1:
                    value = pltpu.roll(f(NR - 1, t), 1, 1)
                elif r == NR:
                    value = pltpu.roll(f(0, t), 127, 1)
                else:
                    value = load(r, t)
                seen[r, t] = value
            return seen[r, t]

        def pair_row(r):
            return {t: f(r, t) + f(r + 1, t - 1) for t in range(first, last + 1)}

        def finish(r, above, here):
            for t in range(first, last):
                out = f(r, t) + (above[t] + here[t + 1])
                if r == 7:
                    out = out * north
                if r == 2:
                    out = out * south
                if t == 7:
                    out = out * west
                if t == 10:
                    out = out * east
                store(r, t, out)

        start = above = pair_row(0)
        for r in range(1, NR):
            here = pair_row(r)
            finish(r, above, here)
            above = here
        finish(0, pair_row(-1), start)


def kernel(
    n_gy,
    n_gx,
    ens,
    cell,
    level,
    innov,
    weight,
    control,
    increment,
    xin,
    cin,
    lin,
    iin,
    win,
    ext,
    xt,
    gt,
    sext,
    spk,
    sst,
    dext,
    grid,
    work,
    ft,
    acc,
    squares,
    image,
    rowa,
    rowb,
    staged,
    sinc,
    in_sem,
    xsend,
    xrecv,
    ssend,
    srecv,
    asend,
    arecv,
    bsend,
    brecv,
    out_sem,
):
    gy = lax.axis_index("gy")
    gx = lax.axis_index("gx")
    lane = lax.broadcasted_iota(jnp.int32, (8, 128), 1)
    sub = lax.broadcasted_iota(jnp.int32, (8, 128), 0)
    block = lane & 7

    loads = [
        pltpu.make_async_copy(src, dst, in_sem.at[i])
        for i, (src, dst) in enumerate(((ens, xin), (cell, cin), (level, lin), (innov, iin), (weight, win)))
    ]
    for load in loads:
        load.start()

    def there(dy, dx):
        return (lax.rem(gy + dy + n_gy, n_gy), lax.rem(gx + dx + n_gx, n_gx))

    def remote(src, dst, send, recv, to):
        return pltpu.make_async_remote_copy(
            src_ref=src, dst_ref=dst, send_sem=send, recv_sem=recv, device_id=to, device_id_type=MESH
        )

    barrier = pltpu.get_barrier_semaphore()
    met = [(0, k) for k in range(1, n_gx)] + [(k, 0) for k in range(1, n_gy)] + list(WAYS[4:])
    for dy, dx in met:
        pl.semaphore_signal(barrier, inc=1, device_id=there(dy, dx), device_id_type=MESH)

    loads[0].wait()

    def widen(i, carry):
        for k in range(4):
            ext[4 * i + k, HALO : HALO + ROWS, :] = xin[4 * i + k].astype(F32)
        return carry

    lax.fori_loop(0, MEMBERS * LEVELS // 4, widen, 0)

    def row_messages(c):
        fields = ext.at[pl.ds(c * PER, PER)]
        return [
            remote(fields.at[:, pl.ds(src, HALO), :], fields.at[:, pl.ds(dst, HALO), :], xsend.at[c, way], xrecv.at[c, way], there(*WAYS[way]))
            for way, (src, dst) in enumerate(((HALO, HALO + ROWS), (ROWS, 0)))
        ]

    def column_messages(c):
        fields = xt.at[c]
        return [
            remote(fields.at[:, pl.ds(src, HALO), :], fields.at[:, pl.ds(dst, HALO), :], xsend.at[c, way], xrecv.at[c, way], there(*WAYS[way]))
            for way, (src, dst) in ((2, (HALO, HALO + COLS)), (3, (COLS, 0)))
        ]

    pl.semaphore_wait(barrier, len(met))
    for c in range(CHUNKS):
        for msg in row_messages(c):
            msg.start()

    for load in loads[1:]:
        load.wait()
    grid[...] = jnp.zeros_like(grid)

    def scatter(k, carry):
        part = pl.ds(pl.multiple_of(k * OBS_STEP, OBS_STEP), OBS_STEP)
        where_at = cin[0, :, part]
        row = where_at >> 7
        col = (where_at & 127) + lin[0, :, part] * COLS
        w = win[0, :, part]
        on_row = lax.broadcasted_iota(jnp.int32, (ROWS, OBS_STEP), 0) == row
        on_col = lax.broadcasted_iota(jnp.int32, (LEVELS * COLS, OBS_STEP), 0) == col
        right = jnp.where(on_col, 1.0, 0.0).astype(BF16)
        left = []
        for value in (w * iin[0, :, part], w):
            for _ in range(3):
                piece = value.astype(BF16).astype(F32)
                left.append(jnp.where(on_row, piece, 0.0).astype(BF16))
                value = value - piece
        left = jnp.concatenate(left, axis=0)
        grid[...] += lax.dot_general(left, right, (((1,), (1,)), ((), ())), preferred_element_type=F32)
        return carry

    lax.fori_loop(0, cin.shape[-1] // OBS_STEP, scatter, 0)
    for lev in range(LEVELS):
        cols = slice(lev * COLS, lev * COLS + COLS)
        grad = grid[0:64, cols] + (grid[64:128, cols] + grid[128:192, cols])
        diag = grid[192:256, cols] + (grid[256:320, cols] + grid[320:384, cols])
        sext[0, lev, HALO : HALO + ROWS, :] = grad * FILTER_SCALE
        dext[lev, 0:HALO, :] = jnp.zeros((HALO, COLS), F32)
        dext[lev, HALO : HALO + ROWS, :] = diag
        dext[lev, HALO + ROWS : EROWS, :] = jnp.zeros((HALO, COLS), F32)

    def state_messages(kind):
        wide, west, east = sext.at[kind], spk.at[kind, 0], spk.at[kind, 1]
        from_west, from_east = sst.at[kind, 0], sst.at[kind, 1]
        pairs = (
            (wide.at[:, pl.ds(HALO, HALO), :], wide.at[:, pl.ds(HALO + ROWS, HALO), :]),
            (wide.at[:, pl.ds(ROWS, HALO), :], wide.at[:, pl.ds(0, HALO), :]),
            (west, from_east.at[pl.ds(HALO, ROWS), :]),
            (east, from_west.at[pl.ds(HALO, ROWS), :]),
            (west.at[pl.ds(0, HALO), :], from_east.at[pl.ds(HALO + ROWS, HALO), :]),
            (east.at[pl.ds(0, HALO), :], from_west.at[pl.ds(HALO + ROWS, HALO), :]),
            (west.at[pl.ds(ROWS - HALO, HALO), :], from_east.at[pl.ds(0, HALO), :]),
            (east.at[pl.ds(ROWS - HALO, HALO), :], from_west.at[pl.ds(0, HALO), :]),
        )
        return [
            remote(src, dst, ssend.at[kind, way], srecv.at[kind, way], there(*WAYS[way]))
            for way, (src, dst) in enumerate(pairs)
        ]

    def share_state(kind):
        for k in range(8):
            at = HALO + 8 * k
            a = sext[kind, 0, at : at + 8, :]
            b = sext[kind, 1, at : at + 8, :]
            spk[kind, 0, 8 * k : 8 * k + 8, :] = jnp.where(lane < 8, a, pltpu.roll(b, 8, 1))
            spk[kind, 1, 8 * k : 8 * k + 8, :] = jnp.where(lane < 8, pltpu.roll(a, 8, 1), pltpu.roll(b, 16, 1))
        msgs = state_messages(kind)
        for msg in msgs:
            msg.start()
        return msgs

    keep_north = jnp.where((gy == 0) & (block == 0), 0.0, 1.0)
    keep_south = jnp.where((gy == n_gy - 1) & (block == 7), 0.0, 1.0)
    keep_west = jnp.where((gx == 0) & (sub == 0), 0.0, 1.0)
    keep_east = jnp.where((gx == n_gx - 1) & (sub == 7), 0.0, 1.0)
    masks = (keep_north, keep_south, keep_west, keep_east)
    near_west = jnp.where((gx == 0) & (sub == 7), 0.0, 1.0)
    near_east = jnp.where((gx == n_gx - 1) & (sub == 0), 0.0, 1.0)

    def turn_state(kind):
        west = by_rows(sst, kind, 0)
        east = by_rows(sst, kind, 1)
        levels = [by_rows(sext, kind, lev) for lev in range(LEVELS)]

        def keep(r, value):
            if r == 7:
                value = value * keep_north
            if r == 2:
                value = value * keep_south
            return value

        for r in range(NR):
            across = jnp.concatenate([levels[0][r], levels[1][r]] * 8, axis=0).T
            for k in range(16):
                gt[r, HALO + 8 * k : HALO + 8 * k + 8, :] = keep(r, across[8 * k : 8 * k + 8])
        for base in (0, 8):
            steps = range(base, min(base + 8, NR))
            both = []
            for lev in range(LEVELS):
                out = jnp.zeros((8, 128), F32)
                for r in steps:
                    at = 16 * (r - base)
                    w = west[r] if at == 8 * lev else pltpu.roll(west[r], (128 + at - 8 * lev) % 128, 1)
                    e = east[r] if at + 8 == 8 * lev else pltpu.roll(east[r], (128 + at + 8 - 8 * lev) % 128, 1)
                    out = jnp.where((lane >= at) & (lane < at + 8), w, out)
                    out = jnp.where((lane >= at + 8) & (lane < at + 16), e, out)
                both.append(out)
            across = jnp.concatenate(both * 8, axis=0).T
            for r in steps:
                at = 16 * (r - base)
                gt[r, 0:8, :] = keep(r, across[at : at + 8] * near_west)
                gt[r, HALO + COLS : ECOLS, :] = keep(r, across[at + 8 : at + 16] * near_east)

    def turn_ensemble(c):
        def one(r, carry):
            across = jnp.concatenate([ext[c * PER + q, pl.ds(r, 8, stride=NR), :] for q in range(PER)], axis=0).T
            xt[c, r, HALO : HALO + COLS, :] = across
            return carry

        lax.fori_loop(0, NR, one, 0)

    def column(ref, t, *lead):
        return ref[(*lead, pl.ds(t, 8, stride=NT), slice(None))]

    def put_column(ref, t, value, *lead):
        ref[(*lead, pl.ds(t, 8, stride=NT), slice(None))] = value

    def apply(kind, c):
        def from_work(i):
            return lambda r, t: work[i, r, 8 * t : 8 * t + 8, :]

        def to_work(i):
            def store(r, t, value):
                work[i, r, 8 * t : 8 * t + 8, :] = value

            return store

        norms = {}

        def to_field(r, t, value):
            put_column(ft, t, value, kind, c, r)
            key = 3 * ((t >= 8) + (t >= 10)) + (r >= 2) + (r >= 8)
            norms[key] = norms[key] + value * value if key in norms else value * value

        def to_image(r, t, value):
            put_column(acc, t, column(acc, t, r) + value * column(xt, t, c, r), r)

        sweep(lambda r, t: column(xt, t, c, r) * column(gt, t, r), to_work(0), masks)
        sweep(from_work(0), to_work(1), masks)
        sweep(from_work(1), to_work(0), masks)
        sweep(from_work(0), to_field, masks)
        for key, value in norms.items():
            squares[kind, key] += value
        sweep(lambda r, t: column(ft, t, kind, c, r), to_work(1), masks)
        sweep(from_work(1), to_work(0), masks)
        sweep(from_work(0), to_work(1), masks)
        sweep(from_work(1), to_image, masks)

    group = lane >> 4

    def state_image(kind):
        def over_members(v):
            v = v + pltpu.roll(v, 16, 1)
            v = v + pltpu.roll(v, 32, 1)
            return v + pltpu.roll(v, 64, 1)

        most, last = [], []
        for k in range(16):
            a = [acc[r, HALO + 8 * k : HALO + 8 * k + 8, :] for r in range(NR)]
            s = a[:8]
            for bit in (1, 2, 4):
                odd = (group & bit) != 0
                s = [jnp.where(odd, s[(i + bit) % 8], s[i]) for i in range(8)]
            s = [s[i] + pltpu.roll(s[i + 1], 16, 1) for i in (0, 2, 4, 6)]
            s = [s[i] + pltpu.roll(s[i + 1], 32, 1) for i in (0, 2)]
            most.append(s[0] + pltpu.roll(s[1], 64, 1))
            last.append(jnp.where(lane < 16, over_members(a[8]), over_members(a[9])))
        most = jnp.concatenate(most, axis=0).T
        last = jnp.concatenate(last, axis=0).T
        for r in range(NR):
            for lev in range(LEVELS):
                at = 16 * (r % 8) + 8 * lev
                value = most[at : at + 8] if r < 8 else last[at : at + 8]
                image[kind, lev, 8 * r : 8 * r + 8, :] = value * FILTER_SCALE

    squares[...] = jnp.zeros_like(squares)
    acc[...] = jnp.zeros_like(acc)
    smsgs = share_state(0)

    def ready(c):
        for msg in row_messages(c):
            msg.wait_recv()
        turn_ensemble(c)
        for msg in column_messages(c):
            msg.start()

    ready(0)
    for msg in smsgs:
        msg.wait_recv()
    turn_state(0)

    def first_pass(c, carry):
        @pl.when(c < CHUNKS)
        def _():
            ready(c)

        for msg in column_messages(c - 1):
            msg.wait_recv()
        apply(0, c - 1)
        return carry

    lax.fori_loop(1, CHUNKS + 1, first_pass, 0)
    state_image(0)

    for lev in range(LEVELS):
        v = [a * b for a, b in zip(tiles(image, 0, lev), by_rows(dext, lev))]
        put_rows(sinc, [a * FILTER_SCALE for a in v], lev)
        sext[1, lev, HALO : HALO + ROWS, :] = sinc[lev, HALO : HALO + ROWS, :]
    vmsgs = share_state(1)
    acc[...] = jnp.zeros_like(acc)
    for msg in vmsgs:
        msg.wait_recv()
    turn_state(1)

    def second_pass(c, carry):
        apply(1, c)
        return carry

    lax.fori_loop(0, CHUNKS, second_pass, 0)
    state_image(1)

    def norm(kind):
        parts = []
        for key in range(9):
            inside = None
            for test in (
                [sub > 0] if key // 3 == 0 else [sub < 7] if key // 3 == 2 else []
            ) + ([block > 0] if key % 3 < 2 else []) + ([block < 7] if key % 3 > 0 else []):
                inside = test if inside is None else inside & test
            parts.append(jnp.where(inside, squares[kind, key], 0.0))
        return jnp.sum(total(parts))

    def weighted(kind):
        parts = []
        for lev in range(LEVELS):
            parts += [b * (a * a) for a, b in zip(tiles(image, kind, lev), by_rows(dext, lev))]
        return jnp.sum(total(parts))

    mine = (norm(0), weighted(0), norm(1), weighted(1))
    line = lane[0:1]
    row = jnp.where(line < 64, jnp.where(line < 32, mine[0], mine[1]), jnp.where(line < 96, mine[2], mine[3]))

    def gather(value, ref, me, n, send, recv, to):
        ref[me] = value
        copies = [remote(ref.at[me], ref.at[me], send.at[k], recv.at[k], to(k)) for k in range(1, n)]
        for copy in copies:
            copy.start()
        for copy in copies:
            copy.wait_recv()
        return copies, jnp.sum(ref[...], axis=0)

    acopies, row = gather(row, rowa, gx, n_gx, asend, arecv, lambda k: there(0, k))
    bcopies, row = gather(row, rowb, gy, n_gy, bsend, brecv, lambda k: there(k, 0))

    sums = [jnp.full((8, 128), jnp.sum(jnp.where(line == 32 * i, row, 0.0)), F32) for i in range(4)]
    bnorm_sq = sums[0] + EPS
    bnorm = jnp.sqrt(bnorm_sq)
    unit, cross, square, cube = [s / bnorm_sq for s in sums]
    alpha_one = unit + cross
    shift = 1.0 - alpha_one
    remain_sq = jnp.maximum(shift * shift * unit + 2.0 * shift * cross + square, 0.0)
    beta_sq = remain_sq + EPS
    beta = jnp.sqrt(beta_sq)
    curve = jnp.maximum(shift * shift * cross + 2.0 * shift * square + cube, 0.0)
    alpha_two = (remain_sq + curve) / beta_sq
    determ = alpha_one * alpha_two - beta_sq
    coef_one = bnorm * alpha_two / determ
    coef_two = -bnorm * beta / determ
    on_base = coef_one / bnorm + coef_two * shift / (bnorm * beta)
    on_grown = coef_two / (bnorm * beta)

    outs = []
    for lev in range(LEVELS):
        x, z = tiles(image, 0, lev), tiles(image, 1, lev)
        put_rows(sinc, [on_base * a + on_grown * b for a, b in zip(x, z)], lev)
    outs.append(pltpu.make_async_copy(sinc.at[:, pl.ds(HALO, ROWS), :], increment, out_sem.at[0]))
    outs[-1].start()

    for c in range(CHUNKS):

        def finish(r, carry):
            mixed = []
            for k in range(16):
                at = slice(HALO + 8 * k, HALO + 8 * k + 8)
                mixed.append(on_base * ft[0, c, r, at, :] + on_grown * ft[1, c, r, at, :])
            mixed = jnp.concatenate(mixed, axis=0).T
            for q in range(PER):
                staged[c * PER + q, pl.ds(r, 8, stride=NR), :] = mixed[8 * q : 8 * q + 8]
            return carry

        lax.fori_loop(0, NR, finish, 0)
        outs.append(
            pltpu.make_async_copy(
                staged.at[pl.ds(c * PER, PER), pl.ds(HALO, ROWS), :], control.at[pl.ds(c * PER, PER)], out_sem.at[1 + c]
            )
        )
        outs[-1].start()
    for out in outs:
        out.wait()
    for c in range(CHUNKS):
        for msg in row_messages(c) + column_messages(c):
            msg.wait_send()
    for msg in smsgs + vmsgs + acopies + bcopies:
        msg.wait_send()


def solution(mesh):
    n_gy, n_gx = mesh.shape["gy"], mesh.shape["gx"]

    def on_device(ensemble, obs_cell, obs_level, innovation, obs_weight):
        obs = obs_cell.shape[-1]
        fields = MEMBERS * LEVELS
        vmem = pltpu.VMEM
        dma = pltpu.SemaphoreType.DMA
        control, increment = pl.pallas_call(
            lambda *refs: kernel(n_gy, n_gx, *refs),
            name="lanczos",
            out_shape=(
                jax.ShapeDtypeStruct((fields, ROWS, COLS), F32),
                jax.ShapeDtypeStruct((LEVELS, ROWS, COLS), F32),
            ),
            in_specs=[pl.BlockSpec(memory_space=pl.ANY)] * 5,
            out_specs=(pl.BlockSpec(memory_space=pl.ANY),) * 2,
            scratch_shapes=[
                vmem((fields, ROWS, COLS), BF16),
                vmem((1, 1, obs), jnp.int32),
                vmem((1, 1, obs), jnp.int32),
                vmem((1, 1, obs), F32),
                vmem((1, 1, obs), F32),
                vmem((fields, EROWS, COLS), F32),
                vmem((CHUNKS, NR, ECOLS, 128), F32),
                vmem((NR, ECOLS, 128), F32),
                vmem((2, LEVELS, EROWS, COLS), F32),
                vmem((2, 2, ROWS, COLS), F32),
                vmem((2, 2, EROWS, COLS), F32),
                vmem((LEVELS, EROWS, COLS), F32),
                vmem((6 * ROWS, LEVELS * COLS), F32),
                vmem((2, NR, ECOLS, 128), F32),
                vmem((2, CHUNKS, NR, ECOLS, 128), F32),
                vmem((NR, ECOLS, 128), F32),
                vmem((2, 9, 8, 128), F32),
                vmem((2, LEVELS, EROWS, COLS), F32),
                vmem((n_gx, 1, COLS), F32),
                vmem((n_gy, 1, COLS), F32),
                vmem((fields, EROWS, COLS), F32),
                vmem((LEVELS, EROWS, COLS), F32),
                dma((5,)),
                dma((CHUNKS, 4)),
                dma((CHUNKS, 4)),
                dma((2, 8)),
                dma((2, 8)),
                dma((n_gx,)),
                dma((n_gx,)),
                dma((n_gy,)),
                dma((n_gy,)),
                dma((1 + CHUNKS,)),
            ],
            compiler_params=pltpu.CompilerParams(
                collective_id=0, has_side_effects=True, vmem_limit_bytes=60 * 1024 * 1024
            ),
        )(ensemble.reshape(fields, ROWS, COLS), obs_cell, obs_level, innovation, obs_weight)
        return control.reshape(MEMBERS, LEVELS, ROWS, COLS), increment

    return jax.shard_map(
        on_device,
        mesh=mesh,
        in_specs=(P(None, None, "gy", "gx"),) + (P("gy", "gx", None),) * 4,
        out_specs=(P(None, None, "gy", "gx"), P(None, "gy", "gx")),
        check_vma=False,
    )
```

```python
import jax
import jax.numpy as jnp
from jax import lax
from jax.experimental import pallas as pl
from jax.experimental.pallas import tpu as pltpu
from jax.sharding import PartitionSpec as P

MESH = pl.DeviceIdType.MESH
F32 = jnp.float32
BF16 = jnp.bfloat16
EPS = 1e-06
FILTER_SCALE = 0.2**4
MEMBERS = 32
LEVELS = 2
ROWS = 64
COLS = 128
HALO = 8
EROWS = ROWS + 2 * HALO
ECOLS = COLS + 2 * HALO
NR = EROWS // 8
NT = ECOLS // 8
CHUNKS = 4
PER = 16
OBS_STEP = 512
BATCHES = 8
BATCH = MEMBERS * LEVELS // BATCHES

WAYS = ((-1, 0), (1, 0), (0, -1), (0, 1), (-1, -1), (-1, 1), (1, -1), (1, 1))


def total(values):
    while len(values) > 1:
        odd = values[len(values) - len(values) % 2 :]
        values = [a + b for a, b in zip(values[0::2], values[1::2])] + odd
    return values[0]


def by_rows(ref, *lead):
    return [ref[(*lead, pl.ds(r, 8, stride=NR), slice(None))] for r in range(NR)]


def put_rows(ref, values, *lead):
    for r in range(NR):
        ref[(*lead, pl.ds(r, 8, stride=NR), slice(None))] = values[r]


def tiles(ref, *lead):
    return [ref[(*lead, slice(8 * r, 8 * r + 8), slice(None))] for r in range(NR)]


def put_tiles(ref, values, *lead):
    for r in range(NR):
        ref[(*lead, slice(8 * r, 8 * r + 8), slice(None))] = values[r]


def halves(x):
    high = x.astype(BF16)
    return jnp.concatenate([high, (x - high.astype(F32)).astype(BF16)], axis=1)


def turned(left, right):
    return lax.dot_general(left, right, (((1,), (1,)), ((), ())), preferred_element_type=F32)


def sweep(load, store, masks):
    north, south, west, east = masks
    for first, last in ((0, NT // 2), (NT // 2, NT)):
        seen = {}

        def f(r, t):
            if (r, t) not in seen:
                if t == -1:
                    value = pltpu.roll(f(r, NT - 1), 1, 0)
                elif t == NT:
                    value = pltpu.roll(f(r, 0), 7, 0)
                elif r == -1:
                    value = pltpu.roll(f(NR - 1, t), 1, 1)
                elif r == NR:
                    value = pltpu.roll(f(0, t), 127, 1)
                else:
                    value = load(r, t)
                seen[r, t] = value
            return seen[r, t]

        def pair_row(r):
            return {t: f(r, t) + f(r + 1, t - 1) for t in range(first, last + 1)}

        def finish(r, above, here):
            for t in range(first, last):
                out = f(r, t) + (above[t] + here[t + 1])
                if r == 7:
                    out = out * north
                if r == 2:
                    out = out * south
                if t == 7:
                    out = out * west
                if t == 10:
                    out = out * east
                store(r, t, out)

        start = above = pair_row(0)
        for r in range(1, NR):
            here = pair_row(r)
            finish(r, above, here)
            above = here
        finish(0, pair_row(-1), start)


def kernel(
    n_gy,
    n_gx,
    ens,
    cell,
    level,
    innov,
    weight,
    base_out,
    grown_out,
    image,
    coef,
    xin,
    cin,
    lin,
    iin,
    win,
    ext,
    xt,
    gt,
    sext,
    spk,
    sst,
    dext,
    grid,
    work,
    ft,
    acc,
    squares,
    rowa,
    rowb,
    in_sem,
    xsend,
    xrecv,
    ssend,
    srecv,
    asend,
    arecv,
    bsend,
    brecv,
):
    gy = lax.axis_index("gy")
    gx = lax.axis_index("gx")
    lane = lax.broadcasted_iota(jnp.int32, (8, 128), 1)
    sub = lax.broadcasted_iota(jnp.int32, (8, 128), 0)
    block = lane & 7
    down = lax.broadcasted_iota(jnp.int32, (128, 128), 0)
    across = lax.broadcasted_iota(jnp.int32, (128, 128), 1)
    unit_one = jnp.where(down == across, 1.0, 0.0).astype(BF16)
    unit_two = jnp.concatenate([unit_one, unit_one], axis=1)
    members = jnp.where(down[:16] == (across[:16] & 15), 1.0, 0.0).astype(BF16)
    members = jnp.concatenate([members, members], axis=1)

    loads = [
        pltpu.make_async_copy(src, dst, in_sem.at[i])
        for i, (src, dst) in enumerate(((ens, xin), (cell, cin), (level, lin), (innov, iin), (weight, win)))
    ]
    for load in loads:
        load.start()

    def there(dy, dx):
        return (lax.rem(gy + dy + n_gy, n_gy), lax.rem(gx + dx + n_gx, n_gx))

    def remote(src, dst, send, recv, to):
        return pltpu.make_async_remote_copy(
            src_ref=src, dst_ref=dst, send_sem=send, recv_sem=recv, device_id=to, device_id_type=MESH
        )

    barrier = pltpu.get_barrier_semaphore()
    met = [(0, k) for k in range(1, n_gx)] + [(k, 0) for k in range(1, n_gy)] + list(WAYS[4:])
    for dy, dx in met:
        pl.semaphore_signal(barrier, inc=1, device_id=there(dy, dx), device_id_type=MESH)

    loads[0].wait()

    def widen(i, carry):
        for k in range(4):
            ext[4 * i + k, HALO : HALO + ROWS, :] = xin[4 * i + k].astype(F32)
        return carry

    lax.fori_loop(0, MEMBERS * LEVELS // 4, widen, 0)

    def row_messages(c):
        fields = ext.at[pl.ds(c * PER, PER)]
        return [
            remote(fields.at[:, pl.ds(src, HALO), :], fields.at[:, pl.ds(dst, HALO), :], xsend.at[c, way], xrecv.at[c, way], there(*WAYS[way]))
            for way, (src, dst) in enumerate(((HALO, HALO + ROWS), (ROWS, 0)))
        ]

    def column_messages(c):
        fields = xt.at[c]
        return [
            remote(fields.at[:, pl.ds(src, HALO), :], fields.at[:, pl.ds(dst, HALO), :], xsend.at[c, way], xrecv.at[c, way], there(*WAYS[way]))
            for way, (src, dst) in ((2, (HALO, HALO + COLS)), (3, (COLS, 0)))
        ]

    pl.semaphore_wait(barrier, len(met))
    for c in range(CHUNKS):
        for msg in row_messages(c):
            msg.start()

    for load in loads[1:]:
        load.wait()
    grid[...] = jnp.zeros_like(grid)

    def scatter(k, carry):
        part = pl.ds(pl.multiple_of(k * OBS_STEP, OBS_STEP), OBS_STEP)
        where_at = cin[0, :, part]
        row = where_at >> 7
        col = (where_at & 127) + lin[0, :, part] * COLS
        w = win[0, :, part]
        on_row = lax.broadcasted_iota(jnp.int32, (ROWS, OBS_STEP), 0) == row
        on_col = lax.broadcasted_iota(jnp.int32, (LEVELS * COLS, OBS_STEP), 0) == col
        right = jnp.where(on_col, 1.0, 0.0).astype(BF16)
        left = []
        for value in (w * iin[0, :, part], w):
            for _ in range(3):
                piece = value.astype(BF16).astype(F32)
                left.append(jnp.where(on_row, piece, 0.0).astype(BF16))
                value = value - piece
        left = jnp.concatenate(left, axis=0)
        grid[...] += lax.dot_general(left, right, (((1,), (1,)), ((), ())), preferred_element_type=F32)
        return carry

    lax.fori_loop(0, cin.shape[-1] // OBS_STEP, scatter, 0)
    for lev in range(LEVELS):
        cols = slice(lev * COLS, lev * COLS + COLS)
        grad = grid[0:64, cols] + (grid[64:128, cols] + grid[128:192, cols])
        diag = grid[192:256, cols] + (grid[256:320, cols] + grid[320:384, cols])
        sext[0, lev, HALO : HALO + ROWS, :] = grad * FILTER_SCALE
        dext[lev, 0:HALO, :] = jnp.zeros((HALO, COLS), F32)
        dext[lev, HALO : HALO + ROWS, :] = diag
        dext[lev, HALO + ROWS : EROWS, :] = jnp.zeros((HALO, COLS), F32)

    def state_messages(kind):
        wide, west, east = sext.at[kind], spk.at[kind, 0], spk.at[kind, 1]
        from_west, from_east = sst.at[kind, 0], sst.at[kind, 1]
        pairs = (
            (wide.at[:, pl.ds(HALO, HALO), :], wide.at[:, pl.ds(HALO + ROWS, HALO), :]),
            (wide.at[:, pl.ds(ROWS, HALO), :], wide.at[:, pl.ds(0, HALO), :]),
            (west, from_east.at[pl.ds(HALO, ROWS), :]),
            (east, from_west.at[pl.ds(HALO, ROWS), :]),
            (west.at[pl.ds(0, HALO), :], from_east.at[pl.ds(HALO + ROWS, HALO), :]),
            (east.at[pl.ds(0, HALO), :], from_west.at[pl.ds(HALO + ROWS, HALO), :]),
            (west.at[pl.ds(ROWS - HALO, HALO), :], from_east.at[pl.ds(0, HALO), :]),
            (east.at[pl.ds(ROWS - HALO, HALO), :], from_west.at[pl.ds(0, HALO), :]),
        )
        return [
            remote(src, dst, ssend.at[kind, way], srecv.at[kind, way], there(*WAYS[way]))
            for way, (src, dst) in enumerate(pairs)
        ]

    def share_state(kind):
        for k in range(8):
            at = HALO + 8 * k
            a = sext[kind, 0, at : at + 8, :]
            b = sext[kind, 1, at : at + 8, :]
            spk[kind, 0, 8 * k : 8 * k + 8, :] = jnp.where(lane < 8, a, pltpu.roll(b, 8, 1))
            spk[kind, 1, 8 * k : 8 * k + 8, :] = jnp.where(lane < 8, pltpu.roll(a, 8, 1), pltpu.roll(b, 16, 1))
        msgs = state_messages(kind)
        for msg in msgs:
            msg.start()
        return msgs

    keep_north = jnp.where((gy == 0) & (block == 0), 0.0, 1.0)
    keep_south = jnp.where((gy == n_gy - 1) & (block == 7), 0.0, 1.0)
    keep_west = jnp.where((gx == 0) & (sub == 0), 0.0, 1.0)
    keep_east = jnp.where((gx == n_gx - 1) & (sub == 7), 0.0, 1.0)
    masks = (keep_north, keep_south, keep_west, keep_east)
    near_west = jnp.where((gx == 0) & (sub == 7), 0.0, 1.0)
    near_east = jnp.where((gx == n_gx - 1) & (sub == 0), 0.0, 1.0)

    def turn_state(kind):
        west = by_rows(sst, kind, 0)
        east = by_rows(sst, kind, 1)
        levels = [by_rows(sext, kind, lev) for lev in range(LEVELS)]

        def keep(r, value):
            if r == 7:
                value = value * keep_north
            if r == 2:
                value = value * keep_south
            return value

        right = []
        for r in range(NR):
            right += [halves(jnp.concatenate([levels[0][r], levels[1][r]], axis=0))] * 8
        for base in (0, 8):
            both = []
            for lev in range(LEVELS):
                out = jnp.zeros((8, 128), F32)
                for r in range(base, min(base + 8, NR)):
                    at = 16 * (r - base)
                    w = west[r] if at == 8 * lev else pltpu.roll(west[r], (128 + at - 8 * lev) % 128, 1)
                    e = east[r] if at + 8 == 8 * lev else pltpu.roll(east[r], (128 + at + 8 - 8 * lev) % 128, 1)
                    out = jnp.where((lane >= at) & (lane < at + 8), w, out)
                    out = jnp.where((lane >= at + 8) & (lane < at + 16), e, out)
                both.append(out)
            right += [halves(jnp.concatenate(both, axis=0))] * 8
        out = turned(unit_two, jnp.concatenate(right, axis=0))
        for r in range(NR):
            for k in range(16):
                gt[r, HALO + 8 * k : HALO + 8 * k + 8, :] = keep(r, out[8 * k : 8 * k + 8, 128 * r : 128 * r + 128])
            at = 16 * (r % 8)
            side = slice(128 * (NR + r // 8), 128 * (NR + r // 8) + 128)
            gt[r, 0:8, :] = keep(r, out[at : at + 8, side] * near_west)
            gt[r, HALO + COLS : ECOLS, :] = keep(r, out[at + 8 : at + 16, side] * near_east)

    def turn_ensemble(c):
        right = [ext[c * PER + q, pl.ds(r, 8, stride=NR), :] for r in range(NR) for q in range(PER)]
        out = turned(unit_one, jnp.concatenate(right, axis=0).astype(BF16))
        for r in range(NR):
            xt[c, r, HALO : HALO + COLS, :] = out[:, 128 * r : 128 * r + 128]

    def column(ref, t, *lead):
        return ref[(*lead, pl.ds(t, 8, stride=NT), slice(None))]

    def put_column(ref, t, value, *lead):
        ref[(*lead, pl.ds(t, 8, stride=NT), slice(None))] = value

    def apply(kind, c):
        def from_work(i):
            return lambda r, t: work[i, r, 8 * t : 8 * t + 8, :]

        def to_work(i):
            def store(r, t, value):
                work[i, r, 8 * t : 8 * t + 8, :] = value

            return store

        norms = {}

        def to_field(r, t, value):
            put_column(ft, t, value, kind, c, r)
            key = 3 * ((t >= 8) + (t >= 10)) + (r >= 2) + (r >= 8)
            norms[key] = norms[key] + value * value if key in norms else value * value

        def to_image(r, t, value):
            put_column(acc, t, column(acc, t, r) + value * column(xt, t, c, r), r)

        sweep(lambda r, t: column(xt, t, c, r) * column(gt, t, r), to_work(0), masks)
        sweep(from_work(0), to_work(1), masks)
        sweep(from_work(1), to_work(0), masks)
        sweep(from_work(0), to_field, masks)
        for key, value in norms.items():
            squares[kind, key] += value
        sweep(lambda r, t: column(ft, t, kind, c, r), to_work(1), masks)
        sweep(from_work(1), to_work(0), masks)
        sweep(from_work(0), to_work(1), masks)
        sweep(from_work(1), to_image, masks)

    def state_image(kind):
        for r in range(NR):
            out = turned(members, halves(acc[r, HALO : HALO + COLS, :])) * FILTER_SCALE
            for lev in range(LEVELS):
                image[kind, lev, pl.ds(r, 8, stride=NR), :] = out[8 * lev : 8 * lev + 8]

    def turn_back(kind, out_ref, chunks):
        def one(i, carry):
            c = i // NR
            r = lax.rem(i, NR)
            out = turned(unit_two, halves(ft[kind, c, r, HALO : HALO + COLS, :]))
            for q in range(PER):
                out_ref[c * PER + q, pl.ds(r, 8, stride=NR), :] = out[8 * q : 8 * q + 8]
            return carry

        lax.fori_loop(chunks[0] * NR, chunks[1] * NR, one, 0, unroll=2)

    squares[...] = jnp.zeros_like(squares)
    acc[...] = jnp.zeros_like(acc)
    smsgs = share_state(0)

    def ready(c):
        for msg in row_messages(c):
            msg.wait_recv()
        turn_ensemble(c)
        for msg in column_messages(c):
            msg.start()

    ready(0)
    for msg in smsgs:
        msg.wait_recv()
    turn_state(0)

    def first_pass(c, carry):
        @pl.when(c < CHUNKS)
        def _():
            ready(c)

        for msg in column_messages(c - 1):
            msg.wait_recv()
        apply(0, c - 1)
        return carry

    lax.fori_loop(1, CHUNKS + 1, first_pass, 0)
    state_image(0)

    for lev in range(LEVELS):
        inner = slice(HALO, HALO + ROWS)
        sext[1, lev, inner, :] = image[0, lev, inner, :] * dext[lev, inner, :] * FILTER_SCALE
    vmsgs = share_state(1)
    acc[...] = jnp.zeros_like(acc)
    turn_back(0, base_out, (0, CHUNKS))
    for msg in vmsgs:
        msg.wait_recv()
    turn_state(1)

    def second_pass(c, carry):
        apply(1, c)
        return carry

    lax.fori_loop(0, CHUNKS, second_pass, 0)
    state_image(1)

    def norm(kind):
        parts = []
        for key in range(9):
            inside = None
            for test in (
                [sub > 0] if key // 3 == 0 else [sub < 7] if key // 3 == 2 else []
            ) + ([block > 0] if key % 3 < 2 else []) + ([block < 7] if key % 3 > 0 else []):
                inside = test if inside is None else inside & test
            parts.append(jnp.where(inside, squares[kind, key], 0.0))
        return jnp.sum(total(parts))

    def weighted(kind):
        parts = []
        for lev in range(LEVELS):
            for k in range(ROWS // 8):
                at = slice(HALO + 8 * k, HALO + 8 * k + 8)
                parts.append(dext[lev, at, :] * (image[kind, lev, at, :] * image[kind, lev, at, :]))
        return jnp.sum(total(parts))

    mine = (norm(0), weighted(0), norm(1), weighted(1))
    line = lane[0:1]
    row = jnp.where(line < 64, jnp.where(line < 32, mine[0], mine[1]), jnp.where(line < 96, mine[2], mine[3]))

    def gather(value, ref, me, n, send, recv, to, chunks):
        ref[me] = value
        copies = [remote(ref.at[me], ref.at[me], send.at[k], recv.at[k], to(k)) for k in range(1, n)]
        for copy in copies:
            copy.start()
        turn_back(1, grown_out, chunks)
        for copy in copies:
            copy.wait_recv()
        return copies, jnp.sum(ref[...], axis=0)

    acopies, row = gather(row, rowa, gx, n_gx, asend, arecv, lambda k: there(0, k), (0, 2))
    bcopies, row = gather(row, rowb, gy, n_gy, bsend, brecv, lambda k: there(k, 0), (2, CHUNKS))

    sums = [jnp.full((8, 128), jnp.sum(jnp.where(line == 32 * i, row, 0.0)), F32) for i in range(4)]
    bnorm_sq = sums[0] + EPS
    bnorm = jnp.sqrt(bnorm_sq)
    unit, cross, square, cube = [s / bnorm_sq for s in sums]
    alpha_one = unit + cross
    shift = 1.0 - alpha_one
    remain_sq = jnp.maximum(shift * shift * unit + 2.0 * shift * cross + square, 0.0)
    beta_sq = remain_sq + EPS
    beta = jnp.sqrt(beta_sq)
    curve = jnp.maximum(shift * shift * cross + 2.0 * shift * square + cube, 0.0)
    alpha_two = (remain_sq + curve) / beta_sq
    determ = alpha_one * alpha_two - beta_sq
    coef_one = bnorm * alpha_two / determ
    coef_two = -bnorm * beta / determ
    on_base = coef_one / bnorm + coef_two * shift / (bnorm * beta)
    on_grown = coef_two / (bnorm * beta)

    coef[0] = on_base
    coef[1] = on_grown
    for c in range(CHUNKS):
        for msg in row_messages(c) + column_messages(c):
            msg.wait_send()
    for msg in smsgs + vmsgs + acopies + bcopies:
        msg.wait_send()


def combine(base, grown, image, coef, control, increment, staged, small, out_sem):
    a, b = coef[0], coef[1]
    copies = []
    for i in range(BATCHES):

        def one(k, carry):
            f = i * BATCH + k
            for r in range(ROWS // 8):
                at = slice(HALO + 8 * r, HALO + 8 * r + 8)
                staged[f, 8 * r : 8 * r + 8, :] = a * base[f, at, :] + b * grown[f, at, :]
            return carry

        lax.fori_loop(0, BATCH, one, 0, unroll=2)
        part = pl.ds(i * BATCH, BATCH)
        copies.append(pltpu.make_async_copy(staged.at[part], control.at[part], out_sem.at[i]))
        copies[-1].start()
    for lev in range(LEVELS):
        for r in range(ROWS // 8):
            at = slice(HALO + 8 * r, HALO + 8 * r + 8)
            small[lev, 8 * r : 8 * r + 8, :] = a * image[0, lev, at, :] + b * image[1, lev, at, :]
    copies.append(pltpu.make_async_copy(small, increment, out_sem.at[BATCHES]))
    copies[-1].start()
    for copy in copies:
        copy.wait()


def solution(mesh):
    n_gy, n_gx = mesh.shape["gy"], mesh.shape["gx"]

    def on_device(ensemble, obs_cell, obs_level, innovation, obs_weight):
        obs = obs_cell.shape[-1]
        fields = MEMBERS * LEVELS
        vmem = pltpu.VMEM
        dma = pltpu.SemaphoreType.DMA
        base, grown, image, coef = pl.pallas_call(
            lambda *refs: kernel(n_gy, n_gx, *refs),
            name="lanczos",
            out_shape=(
                jax.ShapeDtypeStruct((fields, EROWS, COLS), F32),
                jax.ShapeDtypeStruct((fields, EROWS, COLS), F32),
                jax.ShapeDtypeStruct((2, LEVELS, EROWS, COLS), F32),
                jax.ShapeDtypeStruct((2, 8, COLS), F32),
            ),
            in_specs=[pl.BlockSpec(memory_space=pltpu.HBM)] * 5,
            out_specs=(pl.BlockSpec(memory_space=vmem),) * 4,
            scratch_shapes=[
                vmem((fields, ROWS, COLS), BF16),
                vmem((1, 1, obs), jnp.int32),
                vmem((1, 1, obs), jnp.int32),
                vmem((1, 1, obs), F32),
                vmem((1, 1, obs), F32),
                vmem((fields, EROWS, COLS), F32),
                vmem((CHUNKS, NR, ECOLS, 128), F32),
                vmem((NR, ECOLS, 128), F32),
                vmem((2, LEVELS, EROWS, COLS), F32),
                vmem((2, 2, ROWS, COLS), F32),
                vmem((2, 2, EROWS, COLS), F32),
                vmem((LEVELS, EROWS, COLS), F32),
                vmem((6 * ROWS, LEVELS * COLS), F32),
                vmem((2, NR, ECOLS, 128), F32),
                vmem((2, CHUNKS, NR, ECOLS, 128), F32),
                vmem((NR, ECOLS, 128), F32),
                vmem((2, 9, 8, 128), F32),
                vmem((n_gx, 1, COLS), F32),
                vmem((n_gy, 1, COLS), F32),
                dma((5,)),
                dma((CHUNKS, 4)),
                dma((CHUNKS, 4)),
                dma((2, 8)),
                dma((2, 8)),
                dma((n_gx,)),
                dma((n_gx,)),
                dma((n_gy,)),
                dma((n_gy,)),
            ],
            compiler_params=pltpu.CompilerParams(
                collective_id=0, has_side_effects=True, vmem_limit_bytes=28 * 1024 * 1024
            ),
        )(
            *[
                pltpu.with_memory_space_constraint(x, pltpu.HBM)
                for x in (ensemble.reshape(fields, ROWS, COLS), obs_cell, obs_level, innovation, obs_weight)
            ]
        )
        control, increment = pl.pallas_call(
            combine,
            name="combine",
            out_shape=(
                jax.ShapeDtypeStruct((fields, ROWS, COLS), F32),
                jax.ShapeDtypeStruct((LEVELS, ROWS, COLS), F32),
            ),
            in_specs=[pl.BlockSpec(memory_space=vmem)] * 4,
            out_specs=(pl.BlockSpec(memory_space=pltpu.HBM),) * 2,
            scratch_shapes=[
                vmem((fields, ROWS, COLS), F32),
                vmem((LEVELS, ROWS, COLS), F32),
                dma((BATCHES + 1,)),
            ],
            compiler_params=pltpu.CompilerParams(vmem_limit_bytes=12 * 1024 * 1024),
        )(base, grown, image, coef)
        return control.reshape(MEMBERS, LEVELS, ROWS, COLS), increment

    return jax.shard_map(
        on_device,
        mesh=mesh,
        in_specs=(P(None, None, "gy", "gx"),) + (P("gy", "gx", None),) * 4,
        out_specs=(P(None, None, "gy", "gx"), P(None, "gy", "gx")),
        check_vma=False,
    )
```

```python
import jax
import jax.numpy as jnp
from jax import lax
from jax.experimental import pallas as pl
from jax.experimental.pallas import tpu as pltpu
from jax.sharding import PartitionSpec as P

MESH = pl.DeviceIdType.MESH
F32 = jnp.float32
BF16 = jnp.bfloat16
EPS = 1e-06
FILTER_SCALE = 0.2**4
MEMBERS = 32
LEVELS = 2
ROWS = 64
COLS = 128
HALO = 8
EROWS = ROWS + 2 * HALO
ECOLS = COLS + 2 * HALO
NR = EROWS // 8
NT = ECOLS // 8
CHUNKS = 4
PER = 16
OBS_STEP = 512
BATCHES = 8
BATCH = MEMBERS * LEVELS // BATCHES

WAYS = ((-1, 0), (1, 0), (0, -1), (0, 1), (-1, -1), (-1, 1), (1, -1), (1, 1))


def total(values):
    while len(values) > 1:
        odd = values[len(values) - len(values) % 2 :]
        values = [a + b for a, b in zip(values[0::2], values[1::2])] + odd
    return values[0]


def by_rows(ref, *lead):
    return [ref[(*lead, pl.ds(r, 8, stride=NR), slice(None))] for r in range(NR)]


def put_rows(ref, values, *lead):
    for r in range(NR):
        ref[(*lead, pl.ds(r, 8, stride=NR), slice(None))] = values[r]


def tiles(ref, *lead):
    return [ref[(*lead, slice(8 * r, 8 * r + 8), slice(None))] for r in range(NR)]


def put_tiles(ref, values, *lead):
    for r in range(NR):
        ref[(*lead, slice(8 * r, 8 * r + 8), slice(None))] = values[r]


def halves(x):
    high = x.astype(BF16)
    return jnp.concatenate([high, (x - high.astype(F32)).astype(BF16)], axis=1)


def turned(left, right):
    return lax.dot_general(left, right, (((1,), (1,)), ((), ())), preferred_element_type=F32)


def sweep(load, store, masks):
    north, south, west, east = masks
    for first, last in ((0, NT // 2), (NT // 2, NT)):
        seen = {}

        def f(r, t):
            if (r, t) not in seen:
                if t == -1:
                    value = pltpu.roll(f(r, NT - 1), 1, 0)
                elif t == NT:
                    value = pltpu.roll(f(r, 0), 7, 0)
                elif r == -1:
                    value = pltpu.roll(f(NR - 1, t), 1, 1)
                elif r == NR:
                    value = pltpu.roll(f(0, t), 127, 1)
                else:
                    value = load(r, t)
                seen[r, t] = value
            return seen[r, t]

        def pair_row(r):
            return {t: f(r, t) + f(r + 1, t - 1) for t in range(first, last + 1)}

        def finish(r, above, here):
            for t in range(first, last):
                out = f(r, t) + (above[t] + here[t + 1])
                if r == 7:
                    out = out * north
                if r == 2:
                    out = out * south
                if t == 7:
                    out = out * west
                if t == 10:
                    out = out * east
                store(r, t, out)

        start = above = pair_row(0)
        for r in range(1, NR):
            here = pair_row(r)
            finish(r, above, here)
            above = here
        finish(0, pair_row(-1), start)


def kernel(
    n_gy,
    n_gx,
    ens,
    cell,
    level,
    innov,
    weight,
    base_out,
    grown_out,
    image,
    coef,
    xin,
    cin,
    lin,
    iin,
    win,
    ext,
    xt,
    gt,
    sext,
    spk,
    sst,
    dext,
    grid,
    work,
    ft,
    acc,
    squares,
    rowa,
    rowb,
    in_sem,
    xsend,
    xrecv,
    ssend,
    srecv,
    asend,
    arecv,
    bsend,
    brecv,
):
    gy = lax.axis_index("gy")
    gx = lax.axis_index("gx")
    lane = lax.broadcasted_iota(jnp.int32, (8, 128), 1)
    sub = lax.broadcasted_iota(jnp.int32, (8, 128), 0)
    block = lane & 7
    down = lax.broadcasted_iota(jnp.int32, (128, 128), 0)
    across = lax.broadcasted_iota(jnp.int32, (128, 128), 1)
    unit_one = jnp.where(down == across, 1.0, 0.0).astype(BF16)
    unit_two = jnp.concatenate([unit_one, unit_one], axis=1)
    members = jnp.where(down[:16] == (across[:16] & 15), 1.0, 0.0).astype(BF16)
    members = jnp.concatenate([members, members], axis=1)

    loads = [
        pltpu.make_async_copy(src, dst, in_sem.at[i])
        for i, (src, dst) in enumerate(
            [(ens.at[pl.ds(c * PER, PER)], xin.at[pl.ds(c * PER, PER)]) for c in range(CHUNKS)]
            + [(cell, cin), (level, lin), (innov, iin), (weight, win)]
        )
    ]
    for load in loads:
        load.start()

    def there(dy, dx):
        return (lax.rem(gy + dy + n_gy, n_gy), lax.rem(gx + dx + n_gx, n_gx))

    def remote(src, dst, send, recv, to):
        return pltpu.make_async_remote_copy(
            src_ref=src, dst_ref=dst, send_sem=send, recv_sem=recv, device_id=to, device_id_type=MESH
        )

    barrier = pltpu.get_barrier_semaphore()
    met = [(0, k) for k in range(1, n_gx)] + [(k, 0) for k in range(1, n_gy)] + list(WAYS[4:])
    for dy, dx in met:
        pl.semaphore_signal(barrier, inc=1, device_id=there(dy, dx), device_id_type=MESH)

    def widen(c):
        loads[c].wait()

        def one(i, carry):
            for k in range(4):
                f = c * PER + 4 * i + k
                ext[f, HALO : HALO + ROWS, :] = xin[f].astype(F32)
            return carry

        lax.fori_loop(0, PER // 4, one, 0)

    widen(0)

    def row_messages(c):
        fields = ext.at[pl.ds(c * PER, PER)]
        return [
            remote(fields.at[:, pl.ds(src, HALO), :], fields.at[:, pl.ds(dst, HALO), :], xsend.at[c, way], xrecv.at[c, way], there(*WAYS[way]))
            for way, (src, dst) in enumerate(((HALO, HALO + ROWS), (ROWS, 0)))
        ]

    def column_messages(c):
        fields = xt.at[c]
        return [
            remote(fields.at[:, pl.ds(src, HALO), :], fields.at[:, pl.ds(dst, HALO), :], xsend.at[c, way], xrecv.at[c, way], there(*WAYS[way]))
            for way, (src, dst) in ((2, (HALO, HALO + COLS)), (3, (COLS, 0)))
        ]

    pl.semaphore_wait(barrier, len(met))
    for msg in row_messages(0):
        msg.start()
    for c in range(1, CHUNKS):
        widen(c)

    for load in loads[CHUNKS:]:
        load.wait()
    grid[...] = jnp.zeros_like(grid)

    def scatter(k, carry):
        part = pl.ds(pl.multiple_of(k * OBS_STEP, OBS_STEP), OBS_STEP)
        where_at = cin[0, :, part]
        row = where_at >> 7
        col = (where_at & 127) + lin[0, :, part] * COLS
        w = win[0, :, part]
        on_row = lax.broadcasted_iota(jnp.int32, (ROWS, OBS_STEP), 0) == row
        on_col = lax.broadcasted_iota(jnp.int32, (LEVELS * COLS, OBS_STEP), 0) == col
        right = jnp.where(on_col, 1.0, 0.0).astype(BF16)
        left = []
        for value in (w * iin[0, :, part], w):
            for _ in range(3):
                piece = value.astype(BF16).astype(F32)
                left.append(jnp.where(on_row, piece, 0.0).astype(BF16))
                value = value - piece
        left = jnp.concatenate(left, axis=0)
        grid[...] += lax.dot_general(left, right, (((1,), (1,)), ((), ())), preferred_element_type=F32)
        return carry

    lax.fori_loop(0, cin.shape[-1] // OBS_STEP, scatter, 0)
    for lev in range(LEVELS):
        cols = slice(lev * COLS, lev * COLS + COLS)
        grad = grid[0:64, cols] + (grid[64:128, cols] + grid[128:192, cols])
        diag = grid[192:256, cols] + (grid[256:320, cols] + grid[320:384, cols])
        sext[0, lev, HALO : HALO + ROWS, :] = grad * FILTER_SCALE
        dext[lev, 0:HALO, :] = jnp.zeros((HALO, COLS), F32)
        dext[lev, HALO : HALO + ROWS, :] = diag
        dext[lev, HALO + ROWS : EROWS, :] = jnp.zeros((HALO, COLS), F32)

    def state_messages(kind):
        wide, west, east = sext.at[kind], spk.at[kind, 0], spk.at[kind, 1]
        from_west, from_east = sst.at[kind, 0], sst.at[kind, 1]
        pairs = (
            (wide.at[:, pl.ds(HALO, HALO), :], wide.at[:, pl.ds(HALO + ROWS, HALO), :]),
            (wide.at[:, pl.ds(ROWS, HALO), :], wide.at[:, pl.ds(0, HALO), :]),
            (west, from_east.at[pl.ds(HALO, ROWS), :]),
            (east, from_west.at[pl.ds(HALO, ROWS), :]),
            (west.at[pl.ds(0, HALO), :], from_east.at[pl.ds(HALO + ROWS, HALO), :]),
            (east.at[pl.ds(0, HALO), :], from_west.at[pl.ds(HALO + ROWS, HALO), :]),
            (west.at[pl.ds(ROWS - HALO, HALO), :], from_east.at[pl.ds(0, HALO), :]),
            (east.at[pl.ds(ROWS - HALO, HALO), :], from_west.at[pl.ds(0, HALO), :]),
        )
        return [
            remote(src, dst, ssend.at[kind, way], srecv.at[kind, way], there(*WAYS[way]))
            for way, (src, dst) in enumerate(pairs)
        ]

    def share_state(kind):
        for k in range(8):
            at = HALO + 8 * k
            a = sext[kind, 0, at : at + 8, :]
            b = sext[kind, 1, at : at + 8, :]
            spk[kind, 0, 8 * k : 8 * k + 8, :] = jnp.where(lane < 8, a, pltpu.roll(b, 8, 1))
            spk[kind, 1, 8 * k : 8 * k + 8, :] = jnp.where(lane < 8, pltpu.roll(a, 8, 1), pltpu.roll(b, 16, 1))
        msgs = state_messages(kind)
        for msg in msgs:
            msg.start()
        return msgs

    keep_north = jnp.where((gy == 0) & (block == 0), 0.0, 1.0)
    keep_south = jnp.where((gy == n_gy - 1) & (block == 7), 0.0, 1.0)
    keep_west = jnp.where((gx == 0) & (sub == 0), 0.0, 1.0)
    keep_east = jnp.where((gx == n_gx - 1) & (sub == 7), 0.0, 1.0)
    masks = (keep_north, keep_south, keep_west, keep_east)
    near_west = jnp.where((gx == 0) & (sub == 7), 0.0, 1.0)
    near_east = jnp.where((gx == n_gx - 1) & (sub == 0), 0.0, 1.0)

    def turn_state(kind):
        west = by_rows(sst, kind, 0)
        east = by_rows(sst, kind, 1)
        levels = [by_rows(sext, kind, lev) for lev in range(LEVELS)]

        def keep(r, value):
            if r == 7:
                value = value * keep_north
            if r == 2:
                value = value * keep_south
            return value

        right = []
        for r in range(NR):
            right += [halves(jnp.concatenate([levels[0][r], levels[1][r]], axis=0))] * 8
        for base in (0, 8):
            both = []
            for lev in range(LEVELS):
                out = jnp.zeros((8, 128), F32)
                for r in range(base, min(base + 8, NR)):
                    at = 16 * (r - base)
                    w = west[r] if at == 8 * lev else pltpu.roll(west[r], (128 + at - 8 * lev) % 128, 1)
                    e = east[r] if at + 8 == 8 * lev else pltpu.roll(east[r], (128 + at + 8 - 8 * lev) % 128, 1)
                    out = jnp.where((lane >= at) & (lane < at + 8), w, out)
                    out = jnp.where((lane >= at + 8) & (lane < at + 16), e, out)
                both.append(out)
            right += [halves(jnp.concatenate(both, axis=0))] * 8
        out = turned(unit_two, jnp.concatenate(right, axis=0))
        for r in range(NR):
            for k in range(16):
                gt[r, HALO + 8 * k : HALO + 8 * k + 8, :] = keep(r, out[8 * k : 8 * k + 8, 128 * r : 128 * r + 128])
            at = 16 * (r % 8)
            side = slice(128 * (NR + r // 8), 128 * (NR + r // 8) + 128)
            gt[r, 0:8, :] = keep(r, out[at : at + 8, side] * near_west)
            gt[r, HALO + COLS : ECOLS, :] = keep(r, out[at + 8 : at + 16, side] * near_east)

    def turn_ensemble(c):
        right = [ext[c * PER + q, pl.ds(r, 8, stride=NR), :] for r in range(NR) for q in range(PER)]
        out = turned(unit_one, jnp.concatenate(right, axis=0).astype(BF16))
        for r in range(NR):
            xt[c, r, HALO : HALO + COLS, :] = out[:, 128 * r : 128 * r + 128]

    def column(ref, t, *lead):
        return ref[(*lead, pl.ds(t, 8, stride=NT), slice(None))]

    def put_column(ref, t, value, *lead):
        ref[(*lead, pl.ds(t, 8, stride=NT), slice(None))] = value

    def apply(kind, c):
        def from_work(i):
            return lambda r, t: work[i, r, 8 * t : 8 * t + 8, :]

        def to_work(i):
            def store(r, t, value):
                work[i, r, 8 * t : 8 * t + 8, :] = value

            return store

        norms = {}

        def to_field(r, t, value):
            put_column(ft, t, value, kind, c, r)
            key = 3 * ((t >= 8) + (t >= 10)) + (r >= 2) + (r >= 8)
            norms[key] = norms[key] + value * value if key in norms else value * value

        def to_image(r, t, value):
            put_column(acc, t, column(acc, t, r) + value * column(xt, t, c, r), r)

        sweep(lambda r, t: column(xt, t, c, r) * column(gt, t, r), to_work(0), masks)
        sweep(from_work(0), to_work(1), masks)
        sweep(from_work(1), to_work(0), masks)
        sweep(from_work(0), to_field, masks)
        for key, value in norms.items():
            squares[kind, key] += value
        sweep(lambda r, t: column(ft, t, kind, c, r), to_work(1), masks)
        sweep(from_work(1), to_work(0), masks)
        sweep(from_work(0), to_work(1), masks)
        sweep(from_work(1), to_image, masks)

    def state_image(kind):
        for r in range(NR):
            out = turned(members, halves(acc[r, HALO : HALO + COLS, :])) * FILTER_SCALE
            for lev in range(LEVELS):
                image[kind, lev, pl.ds(r, 8, stride=NR), :] = out[8 * lev : 8 * lev + 8]

    def turn_back(kind, chunks):
        out_ref = (base_out, grown_out)[kind]

        def one(i, carry):
            c = i // NR
            r = lax.rem(i, NR)
            out = turned(unit_two, halves(ft[kind, c, r, HALO : HALO + COLS, :]))
            for q in range(PER):
                out_ref[c * PER + q, pl.ds(r, 8, stride=NR), :] = out[8 * q : 8 * q + 8]
            return carry

        lax.fori_loop(chunks[0] * NR, chunks[1] * NR, one, 0, unroll=5)

    smsgs = share_state(0)
    for c in range(1, CHUNKS):
        for msg in row_messages(c):
            msg.start()
    squares[...] = jnp.zeros_like(squares)
    acc[...] = jnp.zeros_like(acc)

    def ready(c):
        for msg in row_messages(c):
            msg.wait_recv()
        turn_ensemble(c)
        for msg in column_messages(c):
            msg.start()

    ready(0)
    for msg in smsgs:
        msg.wait_recv()
    turn_state(0)
    ready(1)

    def first_pass(c, carry):
        for msg in column_messages(c):
            msg.wait_recv()
        apply(0, c)

        @pl.when(c + 2 < CHUNKS)
        def _():
            ready(c + 2)

        return carry

    lax.fori_loop(0, CHUNKS, first_pass, 0)
    state_image(0)

    for lev in range(LEVELS):
        inner = slice(HALO, HALO + ROWS)
        sext[1, lev, inner, :] = image[0, lev, inner, :] * dext[lev, inner, :] * FILTER_SCALE
    vmsgs = share_state(1)
    acc[...] = jnp.zeros_like(acc)
    turn_back(0, (0, 3))
    for msg in vmsgs:
        msg.wait_recv()
    turn_state(1)

    def second_pass(c, carry):
        apply(1, c)
        return carry

    lax.fori_loop(0, CHUNKS, second_pass, 0)
    state_image(1)

    def norm(kind):
        parts = []
        for key in range(9):
            inside = None
            for test in (
                [sub > 0] if key // 3 == 0 else [sub < 7] if key // 3 == 2 else []
            ) + ([block > 0] if key % 3 < 2 else []) + ([block < 7] if key % 3 > 0 else []):
                inside = test if inside is None else inside & test
            parts.append(jnp.where(inside, squares[kind, key], 0.0))
        return jnp.sum(total(parts))

    def weighted(kind):
        parts = []
        for lev in range(LEVELS):
            for k in range(ROWS // 8):
                at = slice(HALO + 8 * k, HALO + 8 * k + 8)
                parts.append(dext[lev, at, :] * (image[kind, lev, at, :] * image[kind, lev, at, :]))
        return jnp.sum(total(parts))

    mine = (norm(0), weighted(0), norm(1), weighted(1))
    line = lane[0:1]
    row = jnp.where(line < 64, jnp.where(line < 32, mine[0], mine[1]), jnp.where(line < 96, mine[2], mine[3]))

    def gather(value, ref, me, n, send, recv, to, fill):
        ref[me] = value
        copies = [remote(ref.at[me], ref.at[me], send.at[k], recv.at[k], to(k)) for k in range(1, n)]
        for copy in copies:
            copy.start()
        for kind, chunks in fill:
            turn_back(kind, chunks)
        for copy in copies:
            copy.wait_recv()
        return copies, jnp.sum(ref[...], axis=0)

    acopies, row = gather(row, rowa, gx, n_gx, asend, arecv, lambda k: there(0, k), [(0, (3, 4)), (1, (0, 1))])
    bcopies, row = gather(row, rowb, gy, n_gy, bsend, brecv, lambda k: there(k, 0), [(1, (1, 4))])

    sums = [jnp.full((8, 128), jnp.sum(jnp.where(line == 32 * i, row, 0.0)), F32) for i in range(4)]
    bnorm_sq = sums[0] + EPS
    bnorm = jnp.sqrt(bnorm_sq)
    unit, cross, square, cube = [s / bnorm_sq for s in sums]
    alpha_one = unit + cross
    shift = 1.0 - alpha_one
    remain_sq = jnp.maximum(shift * shift * unit + 2.0 * shift * cross + square, 0.0)
    beta_sq = remain_sq + EPS
    beta = jnp.sqrt(beta_sq)
    curve = jnp.maximum(shift * shift * cross + 2.0 * shift * square + cube, 0.0)
    alpha_two = (remain_sq + curve) / beta_sq
    determ = alpha_one * alpha_two - beta_sq
    coef_one = bnorm * alpha_two / determ
    coef_two = -bnorm * beta / determ
    on_base = coef_one / bnorm + coef_two * shift / (bnorm * beta)
    on_grown = coef_two / (bnorm * beta)

    coef[0] = on_base
    coef[1] = on_grown
    for c in range(CHUNKS):
        for msg in row_messages(c) + column_messages(c):
            msg.wait_send()
    for msg in smsgs + vmsgs + acopies + bcopies:
        msg.wait_send()


def combine(base, grown, image, coef, control, increment, staged, small, out_sem):
    a, b = coef[0], coef[1]
    copies = []
    for i in range(BATCHES):

        def one(k, carry):
            f = i * BATCH + k
            for r in range(ROWS // 8):
                at = slice(HALO + 8 * r, HALO + 8 * r + 8)
                staged[f, 8 * r : 8 * r + 8, :] = a * base[f, at, :] + b * grown[f, at, :]
            return carry

        lax.fori_loop(0, BATCH, one, 0, unroll=2)
        part = pl.ds(i * BATCH, BATCH)
        copies.append(pltpu.make_async_copy(staged.at[part], control.at[part], out_sem.at[i]))
        copies[-1].start()
    for lev in range(LEVELS):
        for r in range(ROWS // 8):
            at = slice(HALO + 8 * r, HALO + 8 * r + 8)
            small[lev, 8 * r : 8 * r + 8, :] = a * image[0, lev, at, :] + b * image[1, lev, at, :]
    copies.append(pltpu.make_async_copy(small, increment, out_sem.at[BATCHES]))
    copies[-1].start()
    for copy in copies:
        copy.wait()


def solution(mesh):
    n_gy, n_gx = mesh.shape["gy"], mesh.shape["gx"]

    def on_device(ensemble, obs_cell, obs_level, innovation, obs_weight):
        obs = obs_cell.shape[-1]
        fields = MEMBERS * LEVELS
        vmem = pltpu.VMEM
        dma = pltpu.SemaphoreType.DMA
        base, grown, image, coef = pl.pallas_call(
            lambda *refs: kernel(n_gy, n_gx, *refs),
            name="lanczos",
            out_shape=(
                jax.ShapeDtypeStruct((fields, EROWS, COLS), F32),
                jax.ShapeDtypeStruct((fields, EROWS, COLS), F32),
                jax.ShapeDtypeStruct((2, LEVELS, EROWS, COLS), F32),
                jax.ShapeDtypeStruct((2, 8, COLS), F32),
            ),
            in_specs=[pl.BlockSpec(memory_space=pltpu.HBM)] * 5,
            out_specs=(pl.BlockSpec(memory_space=vmem),) * 4,
            scratch_shapes=[
                vmem((fields, ROWS, COLS), BF16),
                vmem((1, 1, obs), jnp.int32),
                vmem((1, 1, obs), jnp.int32),
                vmem((1, 1, obs), F32),
                vmem((1, 1, obs), F32),
                vmem((fields, EROWS, COLS), F32),
                vmem((CHUNKS, NR, ECOLS, 128), F32),
                vmem((NR, ECOLS, 128), F32),
                vmem((2, LEVELS, EROWS, COLS), F32),
                vmem((2, 2, ROWS, COLS), F32),
                vmem((2, 2, EROWS, COLS), F32),
                vmem((LEVELS, EROWS, COLS), F32),
                vmem((6 * ROWS, LEVELS * COLS), F32),
                vmem((2, NR, ECOLS, 128), F32),
                vmem((2, CHUNKS, NR, ECOLS, 128), F32),
                vmem((NR, ECOLS, 128), F32),
                vmem((2, 9, 8, 128), F32),
                vmem((n_gx, 1, COLS), F32),
                vmem((n_gy, 1, COLS), F32),
                dma((CHUNKS + 4,)),
                dma((CHUNKS, 4)),
                dma((CHUNKS, 4)),
                dma((2, 8)),
                dma((2, 8)),
                dma((n_gx,)),
                dma((n_gx,)),
                dma((n_gy,)),
                dma((n_gy,)),
            ],
            compiler_params=pltpu.CompilerParams(
                collective_id=0, has_side_effects=True, vmem_limit_bytes=28 * 1024 * 1024
            ),
        )(
            *[
                pltpu.with_memory_space_constraint(x, pltpu.HBM)
                for x in (ensemble.reshape(fields, ROWS, COLS), obs_cell, obs_level, innovation, obs_weight)
            ]
        )
        control, increment = pl.pallas_call(
            combine,
            name="combine",
            out_shape=(
                jax.ShapeDtypeStruct((fields, ROWS, COLS), F32),
                jax.ShapeDtypeStruct((LEVELS, ROWS, COLS), F32),
            ),
            in_specs=[pl.BlockSpec(memory_space=vmem)] * 4,
            out_specs=(pl.BlockSpec(memory_space=pltpu.HBM),) * 2,
            scratch_shapes=[
                vmem((fields, ROWS, COLS), F32),
                vmem((LEVELS, ROWS, COLS), F32),
                dma((BATCHES + 1,)),
            ],
            compiler_params=pltpu.CompilerParams(vmem_limit_bytes=12 * 1024 * 1024),
        )(base, grown, image, coef)
        return control.reshape(MEMBERS, LEVELS, ROWS, COLS), increment

    return jax.shard_map(
        on_device,
        mesh=mesh,
        in_specs=(P(None, None, "gy", "gx"),) + (P("gy", "gx", None),) * 4,
        out_specs=(P(None, None, "gy", "gx"), P(None, "gy", "gx")),
        check_vma=False,
    )
```

```python
import jax
import jax.numpy as jnp
from jax import lax
from jax.experimental import pallas as pl
from jax.experimental.pallas import tpu as pltpu
from jax.sharding import PartitionSpec as P

MESH = pl.DeviceIdType.MESH
F32 = jnp.float32
BF16 = jnp.bfloat16
EPS = 1e-06
FILTER_SCALE = 0.2**4
MEMBERS = 32
LEVELS = 2
ROWS = 64
COLS = 128
HALO = 8
EROWS = ROWS + 2 * HALO
ECOLS = COLS + 2 * HALO
NR = EROWS // 8
NT = ECOLS // 8
CHUNKS = 4
PER = 16
OBS_STEP = 512
BATCHES = 8
BATCH = MEMBERS * LEVELS // BATCHES

WAYS = ((-1, 0), (1, 0), (0, -1), (0, 1), (-1, -1), (-1, 1), (1, -1), (1, 1))


def total(values):
    while len(values) > 1:
        odd = values[len(values) - len(values) % 2 :]
        values = [a + b for a, b in zip(values[0::2], values[1::2])] + odd
    return values[0]


def by_rows(ref, *lead):
    return [ref[(*lead, pl.ds(r, 8, stride=NR), slice(None))] for r in range(NR)]


def put_rows(ref, values, *lead):
    for r in range(NR):
        ref[(*lead, pl.ds(r, 8, stride=NR), slice(None))] = values[r]


def tiles(ref, *lead):
    return [ref[(*lead, slice(8 * r, 8 * r + 8), slice(None))] for r in range(NR)]


def put_tiles(ref, values, *lead):
    for r in range(NR):
        ref[(*lead, slice(8 * r, 8 * r + 8), slice(None))] = values[r]


def halves(x):
    high = x.astype(BF16)
    return jnp.concatenate([high, (x - high.astype(F32)).astype(BF16)], axis=1)


def turned(left, right):
    return lax.dot_general(left, right, (((1,), (1,)), ((), ())), preferred_element_type=F32)


def sweep(load, store, masks):
    north, south, west, east = masks
    for first, last in ((0, NT // 2), (NT // 2, NT)):
        seen = {}

        def f(r, t):
            if (r, t) not in seen:
                if t == -1:
                    value = pltpu.roll(f(r, NT - 1), 1, 0)
                elif t == NT:
                    value = pltpu.roll(f(r, 0), 7, 0)
                elif r == -1:
                    value = pltpu.roll(f(NR - 1, t), 1, 1)
                elif r == NR:
                    value = pltpu.roll(f(0, t), 127, 1)
                else:
                    value = load(r, t)
                seen[r, t] = value
            return seen[r, t]

        def pair_row(r):
            return {t: f(r, t) + f(r + 1, t - 1) for t in range(first, last + 1)}

        def finish(r, above, here):
            for t in range(first, last):
                out = f(r, t) + (above[t] + here[t + 1])
                if r == 7:
                    out = out * north
                if r == 2:
                    out = out * south
                if t == 7:
                    out = out * west
                if t == 10:
                    out = out * east
                store(r, t, out)

        start = above = pair_row(0)
        for r in range(1, NR):
            here = pair_row(r)
            finish(r, above, here)
            above = here
        finish(0, pair_row(-1), start)


def kernel(
    n_gy,
    n_gx,
    ens,
    cell,
    level,
    innov,
    weight,
    base_out,
    grown_out,
    image,
    coef,
    xin,
    cin,
    lin,
    iin,
    win,
    ext,
    rhalo,
    eside,
    cpack,
    corner,
    xt,
    gt,
    sext,
    spk,
    sthin,
    sland,
    sst,
    dext,
    grid,
    work,
    ft,
    acc,
    squares,
    rowa,
    rowb,
    in_sem,
    xsend,
    xrecv,
    csend,
    crecv,
    ssend,
    srecv,
    asend,
    arecv,
    bsend,
    brecv,
):
    gy = lax.axis_index("gy")
    gx = lax.axis_index("gx")
    lane = lax.broadcasted_iota(jnp.int32, (8, 128), 1)
    sub = lax.broadcasted_iota(jnp.int32, (8, 128), 0)
    block = lane & 7
    down = lax.broadcasted_iota(jnp.int32, (128, 128), 0)
    across = lax.broadcasted_iota(jnp.int32, (128, 128), 1)
    unit_one = jnp.where(down == across, 1.0, 0.0).astype(BF16)
    unit_two = jnp.concatenate([unit_one, unit_one], axis=1)
    members = jnp.where(down[:16] == (across[:16] & 15), 1.0, 0.0).astype(BF16)
    members = jnp.concatenate([members, members], axis=1)

    loads = [
        pltpu.make_async_copy(src, dst, in_sem.at[i])
        for i, (src, dst) in enumerate(
            [(ens.at[pl.ds(c * PER, PER)], xin.at[pl.ds(c * PER, PER)]) for c in range(CHUNKS)]
            + [(cell, cin), (level, lin), (innov, iin), (weight, win)]
        )
    ]
    for load in loads:
        load.start()

    def there(dy, dx):
        return (lax.rem(gy + dy + n_gy, n_gy), lax.rem(gx + dx + n_gx, n_gx))

    def remote(src, dst, send, recv, to):
        return pltpu.make_async_remote_copy(
            src_ref=src, dst_ref=dst, send_sem=send, recv_sem=recv, device_id=to, device_id_type=MESH
        )

    barrier = pltpu.get_barrier_semaphore()
    met = [(0, k) for k in range(1, n_gx)] + [(k, 0) for k in range(1, n_gy)] + list(WAYS[4:])
    for dy, dx in met:
        pl.semaphore_signal(barrier, inc=1, device_id=there(dy, dx), device_id_type=MESH)

    for load in loads[CHUNKS:]:
        load.wait()
    grid[...] = jnp.zeros_like(grid)

    def scatter(k, carry):
        part = pl.ds(pl.multiple_of(k * OBS_STEP, OBS_STEP), OBS_STEP)
        where_at = cin[0, :, part]
        row = where_at >> 7
        col = (where_at & 127) + lin[0, :, part] * COLS
        w = win[0, :, part]
        on_row = lax.broadcasted_iota(jnp.int32, (ROWS, OBS_STEP), 0) == row
        on_col = lax.broadcasted_iota(jnp.int32, (LEVELS * COLS, OBS_STEP), 0) == col
        right = jnp.where(on_col, 1.0, 0.0).astype(BF16)
        left = []
        for value in (w * iin[0, :, part], w):
            for _ in range(2):
                piece = value.astype(BF16).astype(F32)
                left.append(jnp.where(on_row, piece, 0.0).astype(BF16))
                value = value - piece
        left = jnp.concatenate(left, axis=0)
        grid[...] += lax.dot_general(left, right, (((1,), (1,)), ((), ())), preferred_element_type=F32)
        return carry

    lax.fori_loop(0, cin.shape[-1] // OBS_STEP, scatter, 0)
    for lev in range(LEVELS):
        cols = slice(lev * COLS, lev * COLS + COLS)
        grad = grid[0:64, cols] + grid[64:128, cols]
        diag = grid[128:192, cols] + grid[192:256, cols]
        sext[0, lev, HALO : HALO + ROWS, :] = grad * FILTER_SCALE
        dext[lev, 0:HALO, :] = jnp.zeros((HALO, COLS), F32)
        dext[lev, HALO : HALO + ROWS, :] = diag
        dext[lev, HALO + ROWS : EROWS, :] = jnp.zeros((HALO, COLS), F32)

    def widen(c):
        loads[c].wait()

        def one(i, carry):
            for k in range(4):
                f = c * PER + 4 * i + k
                ext[f, 0:HALO, :] = jnp.zeros((HALO, COLS), F32)
                ext[f, HALO + ROWS : EROWS, :] = jnp.zeros((HALO, COLS), F32)
                ext[f, HALO : HALO + ROWS, :] = xin[f].astype(F32)
            return carry

        lax.fori_loop(0, PER // 4, one, 0)

    widen(0)

    def row_messages(c):
        fields = pl.ds(c * PER, PER)
        return [
            remote(ext.at[fields, pl.ds(src, HALO), :], rhalo.at[fields, pl.ds(dst, HALO), :], xsend.at[c, way], xrecv.at[c, way], there(*WAYS[way]))
            for way, (src, dst) in enumerate(((HALO, HALO), (ROWS, 0)))
        ]

    def column_messages(c):
        return [
            remote(eside.at[side, c], xt.at[c, :, pl.ds(dst, HALO), :], xsend.at[c, 2 + side], xrecv.at[c, 2 + side], there(*WAYS[2 + side]))
            for side, dst in ((0, HALO + COLS), (1, 0))
        ]

    def corner_messages():
        return [
            remote(cpack.at[side, :, pl.ds(low, HALO), :], corner.at[3 - k], csend.at[k], crecv.at[k], there(*WAYS[4 + k]))
            for k, (side, low) in enumerate(((0, 0), (1, 0), (0, HALO), (1, HALO)))
        ]

    def reversed_eights(x):
        for width in (1, 2, 4):
            x = jnp.where((lane & width) == 0, pltpu.roll(x, 128 - width, 1), pltpu.roll(x, width, 1))
        return x

    def pack_corners(c, carry):
        for low, at in ((0, HALO), (HALO, ROWS)):
            west = jnp.zeros((8, 128), F32)
            east = jnp.zeros((8, 128), F32)
            for q in range(PER):
                part = ext[c * PER + q, at : at + HALO, :]
                here = (lane >= 8 * q) & (lane < 8 * q + 8)
                west = jnp.where(here, pltpu.roll(part, 8 * q, 1) if q else part, west)
                east = jnp.where(here, pltpu.roll(part, 8 * q + 8, 1) if q < 15 else part, east)
            cpack[0, c, low : low + HALO, :] = reversed_eights(west)
            cpack[1, c, low : low + HALO, :] = reversed_eights(east)
        return carry

    def turn_right(c):
        right = [ext[c * PER + q, pl.ds(r, 8, stride=NR), :] for r in range(NR) for q in range(PER)]
        return jnp.concatenate(right, axis=0).astype(BF16)

    ends = jnp.concatenate([unit_one[0:8].astype(F32), unit_one[120:128].astype(F32)], axis=0).astype(BF16)

    def early_columns(c, carry):
        out = turned(ends, turn_right(c))
        for r in range(NR):
            eside[0, c, r] = out[0:8, 128 * r : 128 * r + 128]
            eside[1, c, r] = out[8:16, 128 * r : 128 * r + 128]
        for msg in column_messages(c):
            msg.start()
        return carry

    def put_corners(c):
        for side, at in ((0, 0), (1, HALO + COLS)):
            for r in range(NR):
                strip = xt[c, r, at : at + HALO, :]
                for which, row, b in ((side, r, 0), (2 + side, r - 2, 7)):
                    if 0 <= row < 8:
                        line = jnp.broadcast_to(corner[which, c, row : row + 1, :], (8, 128))
                        line = pltpu.roll(line, 0 if b else 121, 1, stride=1, stride_axis=0)
                        strip = jnp.where(block == b, line, strip)
                xt[c, r, at : at + HALO, :] = strip

    def state_messages(kind):
        wide, west, east = sext.at[kind], spk.at[kind, 0], spk.at[kind, 1]
        from_west, from_east = sst.at[kind, 0], sst.at[kind, 1]
        pairs = (
            (wide.at[:, pl.ds(HALO, HALO), :], wide.at[:, pl.ds(HALO + ROWS, HALO), :]),
            (wide.at[:, pl.ds(ROWS, HALO), :], wide.at[:, pl.ds(0, HALO), :]),
            (sthin.at[kind, 0], sland.at[kind, 1]),
            (sthin.at[kind, 1], sland.at[kind, 0]),
            (west.at[pl.ds(0, HALO), :], from_east.at[pl.ds(HALO + ROWS, HALO), :]),
            (east.at[pl.ds(0, HALO), :], from_west.at[pl.ds(HALO + ROWS, HALO), :]),
            (west.at[pl.ds(HALO, HALO), :], from_east.at[pl.ds(0, HALO), :]),
            (east.at[pl.ds(HALO, HALO), :], from_west.at[pl.ds(0, HALO), :]),
        )
        return [
            remote(src, dst, ssend.at[kind, way], srecv.at[kind, way], there(*WAYS[way]))
            for way, (src, dst) in enumerate(pairs)
        ]

    def share_state(kind):
        thin = [jnp.zeros((8, 128), F32)] * 2
        for k in range(8):
            at = HALO + 8 * k
            a = sext[kind, 0, at : at + 8, :]
            b = sext[kind, 1, at : at + 8, :]
            here = (lane >= 16 * k) & (lane < 16 * k + 8)
            both = (lane >= 16 * k) & (lane < 16 * k + 16)
            for side in range(2):
                first = (16 * k + 8 * side) % 128
                x = jnp.where(here, pltpu.roll(a, first, 1) if first else a, pltpu.roll(b, (first + 8) % 128, 1) if first != 120 else b)
                thin[side] = jnp.where(both, x, thin[side])
        for side in range(2):
            sthin[kind, side] = thin[side]
            spk[kind, side, 0:8, :] = thin[side]
            spk[kind, side, 8:16, :] = pltpu.roll(thin[side], 16, 1)
        msgs = state_messages(kind)
        for msg in msgs:
            msg.start()
        return msgs

    keep_north = jnp.where((gy == 0) & (block == 0), 0.0, 1.0)
    keep_south = jnp.where((gy == n_gy - 1) & (block == 7), 0.0, 1.0)
    keep_west = jnp.where((gx == 0) & (sub == 0), 0.0, 1.0)
    keep_east = jnp.where((gx == n_gx - 1) & (sub == 7), 0.0, 1.0)
    masks = (keep_north, keep_south, keep_west, keep_east)
    near_west = jnp.where((gx == 0) & (sub == 7), 0.0, 1.0)
    near_east = jnp.where((gx == n_gx - 1) & (sub == 0), 0.0, 1.0)

    def turn_state(kind):
        for side in range(2):
            thin = sland[kind, side]
            for k in range(8):
                sst[kind, side, HALO + 8 * k : 2 * HALO + 8 * k, :] = pltpu.roll(thin, 128 - 16 * k, 1) if k else thin
        west = by_rows(sst, kind, 0)
        east = by_rows(sst, kind, 1)
        levels = [by_rows(sext, kind, lev) for lev in range(LEVELS)]

        def keep(r, value):
            if r == 7:
                value = value * keep_north
            if r == 2:
                value = value * keep_south
            return value

        right = []
        for r in range(NR):
            right += [halves(jnp.concatenate([levels[0][r], levels[1][r]], axis=0))] * 8
        for base in (0, 8):
            both = []
            for lev in range(LEVELS):
                out = jnp.zeros((8, 128), F32)
                for r in range(base, min(base + 8, NR)):
                    at = 16 * (r - base)
                    w = west[r] if at == 8 * lev else pltpu.roll(west[r], (128 + at - 8 * lev) % 128, 1)
                    e = east[r] if at + 8 == 8 * lev else pltpu.roll(east[r], (128 + at + 8 - 8 * lev) % 128, 1)
                    out = jnp.where((lane >= at) & (lane < at + 8), w, out)
                    out = jnp.where((lane >= at + 8) & (lane < at + 16), e, out)
                both.append(out)
            right += [halves(jnp.concatenate(both, axis=0))] * 8
        out = turned(unit_two, jnp.concatenate(right, axis=0))
        for r in range(NR):
            for k in range(16):
                gt[r, HALO + 8 * k : HALO + 8 * k + 8, :] = keep(r, out[8 * k : 8 * k + 8, 128 * r : 128 * r + 128])
            at = 16 * (r % 8)
            side = slice(128 * (NR + r // 8), 128 * (NR + r // 8) + 128)
            gt[r, 0:8, :] = keep(r, out[at : at + 8, side] * near_west)
            gt[r, HALO + COLS : ECOLS, :] = keep(r, out[at + 8 : at + 16, side] * near_east)

    def turn_ensemble(c):
        for q in range(PER):
            f = c * PER + q
            ext[f, 0:HALO, :] = rhalo[f, 0:HALO, :]
            ext[f, HALO + ROWS : EROWS, :] = rhalo[f, HALO : 2 * HALO, :]
        out = turned(unit_one, turn_right(c))
        for r in range(NR):
            xt[c, r, HALO : HALO + COLS, :] = out[:, 128 * r : 128 * r + 128]

    def column(ref, t, *lead):
        return ref[(*lead, pl.ds(t, 8, stride=NT), slice(None))]

    def put_column(ref, t, value, *lead):
        ref[(*lead, pl.ds(t, 8, stride=NT), slice(None))] = value

    def apply(kind, c):
        def from_work(i):
            return lambda r, t: work[i, r, 8 * t : 8 * t + 8, :]

        def to_work(i):
            def store(r, t, value):
                work[i, r, 8 * t : 8 * t + 8, :] = value

            return store

        norms = {}

        def to_field(r, t, value):
            put_column(ft, t, value, kind, c, r)
            key = 3 * ((t >= 8) + (t >= 10)) + (r >= 2) + (r >= 8)
            norms[key] = norms[key] + value * value if key in norms else value * value

        def to_image(r, t, value):
            put_column(acc, t, column(acc, t, r) + value * column(xt, t, c, r), r)

        sweep(lambda r, t: column(xt, t, c, r) * column(gt, t, r), to_work(0), masks)
        sweep(from_work(0), to_work(1), masks)
        sweep(from_work(1), to_work(0), masks)
        sweep(from_work(0), to_field, masks)
        for key, value in norms.items():
            squares[kind, key] += value
        sweep(lambda r, t: column(ft, t, kind, c, r), to_work(1), masks)
        sweep(from_work(1), to_work(0), masks)
        sweep(from_work(0), to_work(1), masks)
        sweep(from_work(1), to_image, masks)

    def state_image(kind):
        for r in range(NR):
            out = turned(members, halves(acc[r, HALO : HALO + COLS, :])) * FILTER_SCALE
            for lev in range(LEVELS):
                image[kind, lev, pl.ds(r, 8, stride=NR), :] = out[8 * lev : 8 * lev + 8]

    def turn_back(kind, chunks):
        out_ref = (base_out, grown_out)[kind]

        def one(i, carry):
            c = i // NR
            r = lax.rem(i, NR)
            out = turned(unit_two, halves(ft[kind, c, r, HALO : HALO + COLS, :]))
            for q in range(PER):
                out_ref[c * PER + q, pl.ds(r, 8, stride=NR), :] = out[8 * q : 8 * q + 8]
            return carry

        lax.fori_loop(chunks[0] * NR, chunks[1] * NR, one, 0, unroll=5)

    pl.semaphore_wait(barrier, len(met))
    for msg in row_messages(0):
        msg.start()
    smsgs = share_state(0)
    widen(1)
    for msg in row_messages(1):
        msg.start()
    for c in range(2, CHUNKS):
        widen(c)
    lax.fori_loop(0, CHUNKS, pack_corners, 0)
    for msg in corner_messages():
        msg.start()
    lax.fori_loop(0, CHUNKS, early_columns, 0)
    for c in range(2, CHUNKS):
        for msg in row_messages(c):
            msg.start()
    squares[...] = jnp.zeros_like(squares)
    acc[...] = jnp.zeros_like(acc)

    for msg in smsgs:
        msg.wait_recv()
    turn_state(0)
    for msg in corner_messages():
        msg.wait_recv()

    def first_pass(c, carry):
        for msg in column_messages(c):
            msg.wait_recv()
        put_corners(c)
        for msg in row_messages(c):
            msg.wait_recv()
        turn_ensemble(c)
        apply(0, c)
        return carry

    lax.fori_loop(0, CHUNKS, first_pass, 0)
    state_image(0)

    for lev in range(LEVELS):
        inner = slice(HALO, HALO + ROWS)
        sext[1, lev, inner, :] = image[0, lev, inner, :] * dext[lev, inner, :] * FILTER_SCALE
    vmsgs = share_state(1)
    acc[...] = jnp.zeros_like(acc)
    turn_back(0, (0, 3))
    for msg in vmsgs:
        msg.wait_recv()
    turn_state(1)

    def second_pass(c, carry):
        apply(1, c)
        return carry

    lax.fori_loop(0, CHUNKS, second_pass, 0)
    state_image(1)

    def norm(kind):
        parts = []
        for key in range(9):
            inside = None
            for test in (
                [sub > 0] if key // 3 == 0 else [sub < 7] if key // 3 == 2 else []
            ) + ([block > 0] if key % 3 < 2 else []) + ([block < 7] if key % 3 > 0 else []):
                inside = test if inside is None else inside & test
            parts.append(jnp.where(inside, squares[kind, key], 0.0))
        return jnp.sum(total(parts))

    def weighted(kind):
        parts = []
        for lev in range(LEVELS):
            for k in range(ROWS // 8):
                at = slice(HALO + 8 * k, HALO + 8 * k + 8)
                parts.append(dext[lev, at, :] * (image[kind, lev, at, :] * image[kind, lev, at, :]))
        return jnp.sum(total(parts))

    mine = (norm(0), weighted(0), norm(1), weighted(1))
    line = lane[0:1]
    row = jnp.where(line < 64, jnp.where(line < 32, mine[0], mine[1]), jnp.where(line < 96, mine[2], mine[3]))

    def gather(value, ref, me, n, send, recv, to, fill):
        ref[me] = value
        copies = [remote(ref.at[me], ref.at[me], send.at[k], recv.at[k], to(k)) for k in range(1, n)]
        for copy in copies:
            copy.start()
        for kind, chunks in fill:
            turn_back(kind, chunks)
        for copy in copies:
            copy.wait_recv()
        return copies, jnp.sum(ref[...], axis=0)

    acopies, row = gather(row, rowa, gx, n_gx, asend, arecv, lambda k: there(0, k), [(0, (3, 4)), (1, (0, 1))])
    bcopies, row = gather(row, rowb, gy, n_gy, bsend, brecv, lambda k: there(k, 0), [(1, (1, 4))])

    sums = [jnp.full((8, 128), jnp.sum(jnp.where(line == 32 * i, row, 0.0)), F32) for i in range(4)]
    bnorm_sq = sums[0] + EPS
    bnorm = jnp.sqrt(bnorm_sq)
    unit, cross, square, cube = [s / bnorm_sq for s in sums]
    alpha_one = unit + cross
    shift = 1.0 - alpha_one
    remain_sq = jnp.maximum(shift * shift * unit + 2.0 * shift * cross + square, 0.0)
    beta_sq = remain_sq + EPS
    beta = jnp.sqrt(beta_sq)
    curve = jnp.maximum(shift * shift * cross + 2.0 * shift * square + cube, 0.0)
    alpha_two = (remain_sq + curve) / beta_sq
    determ = alpha_one * alpha_two - beta_sq
    coef_one = bnorm * alpha_two / determ
    coef_two = -bnorm * beta / determ
    on_base = coef_one / bnorm + coef_two * shift / (bnorm * beta)
    on_grown = coef_two / (bnorm * beta)

    coef[0] = on_base
    coef[1] = on_grown
    for c in range(CHUNKS):
        for msg in row_messages(c) + column_messages(c):
            msg.wait_send()
    for msg in corner_messages() + smsgs + vmsgs + acopies + bcopies:
        msg.wait_send()


def combine(base, grown, image, coef, control, increment, staged, small, out_sem):
    a, b = coef[0], coef[1]
    copies = []
    for i in range(BATCHES):

        def one(k, carry):
            f = i * BATCH + k
            for r in range(ROWS // 8):
                at = slice(HALO + 8 * r, HALO + 8 * r + 8)
                staged[f, 8 * r : 8 * r + 8, :] = a * base[f, at, :] + b * grown[f, at, :]
            return carry

        lax.fori_loop(0, BATCH, one, 0, unroll=2)
        part = pl.ds(i * BATCH, BATCH)
        copies.append(pltpu.make_async_copy(staged.at[part], control.at[part], out_sem.at[i]))
        copies[-1].start()
    for lev in range(LEVELS):
        for r in range(ROWS // 8):
            at = slice(HALO + 8 * r, HALO + 8 * r + 8)
            small[lev, 8 * r : 8 * r + 8, :] = a * image[0, lev, at, :] + b * image[1, lev, at, :]
    copies.append(pltpu.make_async_copy(small, increment, out_sem.at[BATCHES]))
    copies[-1].start()
    for copy in copies:
        copy.wait()


def solution(mesh):
    n_gy, n_gx = mesh.shape["gy"], mesh.shape["gx"]

    def on_device(ensemble, obs_cell, obs_level, innovation, obs_weight):
        obs = obs_cell.shape[-1]
        fields = MEMBERS * LEVELS
        vmem = pltpu.VMEM
        dma = pltpu.SemaphoreType.DMA
        base, grown, image, coef = pl.pallas_call(
            lambda *refs: kernel(n_gy, n_gx, *refs),
            name="lanczos",
            out_shape=(
                jax.ShapeDtypeStruct((fields, EROWS, COLS), F32),
                jax.ShapeDtypeStruct((fields, EROWS, COLS), F32),
                jax.ShapeDtypeStruct((2, LEVELS, EROWS, COLS), F32),
                jax.ShapeDtypeStruct((2, 8, COLS), F32),
            ),
            in_specs=[pl.BlockSpec(memory_space=pltpu.HBM)] * 5,
            out_specs=(pl.BlockSpec(memory_space=vmem),) * 4,
            scratch_shapes=[
                vmem((fields, ROWS, COLS), BF16),
                vmem((1, 1, obs), jnp.int32),
                vmem((1, 1, obs), jnp.int32),
                vmem((1, 1, obs), F32),
                vmem((1, 1, obs), F32),
                vmem((fields, EROWS, COLS), F32),
                vmem((fields, 2 * HALO, COLS), F32),
                vmem((2, CHUNKS, NR, HALO, 128), F32),
                vmem((2, CHUNKS, 2 * HALO, 128), F32),
                vmem((4, CHUNKS, HALO, 128), F32),
                vmem((CHUNKS, NR, ECOLS, 128), F32),
                vmem((NR, ECOLS, 128), F32),
                vmem((2, LEVELS, EROWS, COLS), F32),
                vmem((2, 2, 2 * HALO, COLS), F32),
                vmem((2, 2, HALO, COLS), F32),
                vmem((2, 2, HALO, COLS), F32),
                vmem((2, 2, EROWS, COLS), F32),
                vmem((LEVELS, EROWS, COLS), F32),
                vmem((4 * ROWS, LEVELS * COLS), F32),
                vmem((2, NR, ECOLS, 128), F32),
                vmem((2, CHUNKS, NR, ECOLS, 128), F32),
                vmem((NR, ECOLS, 128), F32),
                vmem((2, 9, 8, 128), F32),
                vmem((n_gx, 1, COLS), F32),
                vmem((n_gy, 1, COLS), F32),
                dma((CHUNKS + 4,)),
                dma((CHUNKS, 4)),
                dma((CHUNKS, 4)),
                dma((4,)),
                dma((4,)),
                dma((2, 8)),
                dma((2, 8)),
                dma((n_gx,)),
                dma((n_gx,)),
                dma((n_gy,)),
                dma((n_gy,)),
            ],
            compiler_params=pltpu.CompilerParams(
                collective_id=0, has_side_effects=True, vmem_limit_bytes=28 * 1024 * 1024
            ),
        )(
            *[
                pltpu.with_memory_space_constraint(x, pltpu.HBM)
                for x in (ensemble.reshape(fields, ROWS, COLS), obs_cell, obs_level, innovation, obs_weight)
            ]
        )
        control, increment = pl.pallas_call(
            combine,
            name="combine",
            out_shape=(
                jax.ShapeDtypeStruct((fields, ROWS, COLS), F32),
                jax.ShapeDtypeStruct((LEVELS, ROWS, COLS), F32),
            ),
            in_specs=[pl.BlockSpec(memory_space=vmem)] * 4,
            out_specs=(pl.BlockSpec(memory_space=pltpu.HBM),) * 2,
            scratch_shapes=[
                vmem((fields, ROWS, COLS), F32),
                vmem((LEVELS, ROWS, COLS), F32),
                dma((BATCHES + 1,)),
            ],
            compiler_params=pltpu.CompilerParams(vmem_limit_bytes=12 * 1024 * 1024),
        )(base, grown, image, coef)
        return control.reshape(MEMBERS, LEVELS, ROWS, COLS), increment

    return jax.shard_map(
        on_device,
        mesh=mesh,
        in_specs=(P(None, None, "gy", "gx"),) + (P("gy", "gx", None),) * 4,
        out_specs=(P(None, None, "gy", "gx"), P(None, "gy", "gx")),
        check_vma=False,
    )
```

```python
import jax
import jax.numpy as jnp
from jax import lax
from jax.experimental import pallas as pl
from jax.experimental.pallas import tpu as pltpu
from jax.sharding import PartitionSpec as P

MESH = pl.DeviceIdType.MESH
F32 = jnp.float32
BF16 = jnp.bfloat16
EPS = 1e-06
FILTER_SCALE = 0.2**4
MEMBERS = 32
LEVELS = 2
ROWS = 64
COLS = 128
HALO = 8
EROWS = ROWS + 2 * HALO
ECOLS = COLS + 2 * HALO
NR = EROWS // 8
NT = ECOLS // 8
CHUNKS = 4
PER = 16
OBS_STEP = 512
BATCHES = 8
BATCH = MEMBERS * LEVELS // BATCHES

WAYS = ((-1, 0), (1, 0), (0, -1), (0, 1), (-1, -1), (-1, 1), (1, -1), (1, 1))


def total(values):
    while len(values) > 1:
        odd = values[len(values) - len(values) % 2 :]
        values = [a + b for a, b in zip(values[0::2], values[1::2])] + odd
    return values[0]


def by_rows(ref, *lead):
    return [ref[(*lead, pl.ds(r, 8, stride=NR), slice(None))] for r in range(NR)]


def put_rows(ref, values, *lead):
    for r in range(NR):
        ref[(*lead, pl.ds(r, 8, stride=NR), slice(None))] = values[r]


def tiles(ref, *lead):
    return [ref[(*lead, slice(8 * r, 8 * r + 8), slice(None))] for r in range(NR)]


def put_tiles(ref, values, *lead):
    for r in range(NR):
        ref[(*lead, slice(8 * r, 8 * r + 8), slice(None))] = values[r]


def halves(x):
    high = x.astype(BF16)
    return jnp.concatenate([high, (x - high.astype(F32)).astype(BF16)], axis=1)


def turned(left, right):
    return lax.dot_general(left, right, (((1,), (1,)), ((), ())), preferred_element_type=F32)


def sweep(load, store, masks):
    north, south, west, east = masks
    for first, last in ((0, NT // 2), (NT // 2, NT)):
        seen = {}

        def f(r, t):
            if (r, t) not in seen:
                if t == -1:
                    value = pltpu.roll(f(r, NT - 1), 1, 0)
                elif t == NT:
                    value = pltpu.roll(f(r, 0), 7, 0)
                elif r == -1:
                    value = pltpu.roll(f(NR - 1, t), 1, 1)
                elif r == NR:
                    value = pltpu.roll(f(0, t), 127, 1)
                else:
                    value = load(r, t)
                seen[r, t] = value
            return seen[r, t]

        def pair_row(r):
            return {t: f(r, t) + f(r + 1, t - 1) for t in range(first, last + 1)}

        def finish(r, above, here):
            for t in range(first, last):
                out = f(r, t) + (above[t] + here[t + 1])
                if r == 7:
                    out = out * north
                if r == 2:
                    out = out * south
                if t == 7:
                    out = out * west
                if t == 10:
                    out = out * east
                store(r, t, out)

        start = above = pair_row(0)
        for r in range(1, NR):
            here = pair_row(r)
            finish(r, above, here)
            above = here
        finish(0, pair_row(-1), start)


def kernel(
    n_gy,
    n_gx,
    ens,
    cell,
    level,
    innov,
    weight,
    base_out,
    grown_out,
    image,
    coef,
    xin,
    cin,
    lin,
    iin,
    win,
    ext,
    rhalo,
    eside,
    cpack,
    corner,
    xt,
    gt,
    sext,
    spk,
    sthin,
    sland,
    sst,
    dext,
    grid,
    work,
    ft,
    acc,
    squares,
    rowa,
    rowb,
    in_sem,
    xsend,
    xrecv,
    csend,
    crecv,
    ssend,
    srecv,
    asend,
    arecv,
    bsend,
    brecv,
):
    gy = lax.axis_index("gy")
    gx = lax.axis_index("gx")
    lane = lax.broadcasted_iota(jnp.int32, (8, 128), 1)
    sub = lax.broadcasted_iota(jnp.int32, (8, 128), 0)
    block = lane & 7
    down = lax.broadcasted_iota(jnp.int32, (128, 128), 0)
    across = lax.broadcasted_iota(jnp.int32, (128, 128), 1)
    unit_one = jnp.where(down == across, 1.0, 0.0).astype(BF16)
    unit_two = jnp.concatenate([unit_one, unit_one], axis=1)
    members = jnp.where(down[:16] == (across[:16] & 15), 1.0, 0.0).astype(BF16)
    members = jnp.concatenate([members, members], axis=1)

    loads = [
        pltpu.make_async_copy(src, dst, in_sem.at[i])
        for i, (src, dst) in enumerate(
            [(ens.at[pl.ds(c * PER, PER)], xin.at[pl.ds(c * PER, PER)]) for c in range(CHUNKS)]
            + [(cell, cin), (level, lin), (innov, iin), (weight, win)]
        )
    ]
    for load in loads:
        load.start()

    def there(dy, dx):
        return (lax.rem(gy + dy + n_gy, n_gy), lax.rem(gx + dx + n_gx, n_gx))

    def remote(src, dst, send, recv, to):
        return pltpu.make_async_remote_copy(
            src_ref=src, dst_ref=dst, send_sem=send, recv_sem=recv, device_id=to, device_id_type=MESH
        )

    barrier = pltpu.get_barrier_semaphore()
    met = [(0, k) for k in range(1, n_gx)] + [(k, 0) for k in range(1, n_gy)] + list(WAYS[4:])
    for dy, dx in met:
        pl.semaphore_signal(barrier, inc=1, device_id=there(dy, dx), device_id_type=MESH)

    for load in loads[CHUNKS:]:
        load.wait()
    grid[...] = jnp.zeros_like(grid)

    def scatter(k, carry):
        part = pl.ds(pl.multiple_of(k * OBS_STEP, OBS_STEP), OBS_STEP)
        where_at = cin[0, :, part]
        row = where_at >> 7
        col = (where_at & 127) + lin[0, :, part] * COLS
        w = win[0, :, part]
        on_row = lax.broadcasted_iota(jnp.int32, (ROWS, OBS_STEP), 0) == row
        on_col = lax.broadcasted_iota(jnp.int32, (LEVELS * COLS, OBS_STEP), 0) == col
        right = jnp.where(on_col, 1.0, 0.0).astype(BF16)
        left = []
        for value in (w * iin[0, :, part], w):
            for _ in range(2):
                piece = value.astype(BF16).astype(F32)
                left.append(jnp.where(on_row, piece, 0.0).astype(BF16))
                value = value - piece
        left = jnp.concatenate(left, axis=0)
        grid[...] += lax.dot_general(left, right, (((1,), (1,)), ((), ())), preferred_element_type=F32)
        return carry

    lax.fori_loop(0, cin.shape[-1] // OBS_STEP, scatter, 0)
    for lev in range(LEVELS):
        cols = slice(lev * COLS, lev * COLS + COLS)
        grad = grid[0:64, cols] + grid[64:128, cols]
        diag = grid[128:192, cols] + grid[192:256, cols]
        sext[0, lev, HALO : HALO + ROWS, :] = grad * FILTER_SCALE
        dext[lev, 0:HALO, :] = jnp.zeros((HALO, COLS), F32)
        dext[lev, HALO : HALO + ROWS, :] = diag
        dext[lev, HALO + ROWS : EROWS, :] = jnp.zeros((HALO, COLS), F32)

    def widen(c):
        loads[c].wait()

        def one(i, carry):
            for k in range(4):
                f = c * PER + 4 * i + k
                ext[f, 0:HALO, :] = jnp.zeros((HALO, COLS), F32)
                ext[f, HALO + ROWS : EROWS, :] = jnp.zeros((HALO, COLS), F32)
                ext[f, HALO : HALO + ROWS, :] = xin[f].astype(F32)
            return carry

        lax.fori_loop(0, PER // 4, one, 0)

    widen(0)

    def row_messages(c):
        fields = pl.ds(c * PER, PER)
        return [
            remote(ext.at[fields, pl.ds(src, HALO), :], rhalo.at[fields, pl.ds(dst, HALO), :], xsend.at[c, way], xrecv.at[c, way], there(*WAYS[way]))
            for way, (src, dst) in enumerate(((HALO, HALO), (ROWS, 0)))
        ]

    def column_messages(c):
        return [
            remote(eside.at[side, c], xt.at[c, :, pl.ds(dst, HALO), :], xsend.at[c, 2 + side], xrecv.at[c, 2 + side], there(*WAYS[2 + side]))
            for side, dst in ((0, HALO + COLS), (1, 0))
        ]

    def corner_messages():
        return [
            remote(cpack.at[side, :, pl.ds(low, HALO), :], corner.at[3 - k], csend.at[k], crecv.at[k], there(*WAYS[4 + k]))
            for k, (side, low) in enumerate(((0, 0), (1, 0), (0, HALO), (1, HALO)))
        ]

    def reversed_eights(x):
        for width in (1, 2, 4):
            x = jnp.where((lane & width) == 0, pltpu.roll(x, 128 - width, 1), pltpu.roll(x, width, 1))
        return x

    def pack_corners(c, carry):
        for low, at in ((0, HALO), (HALO, ROWS)):
            west = jnp.zeros((8, 128), F32)
            east = jnp.zeros((8, 128), F32)
            for q in range(PER):
                part = ext[c * PER + q, at : at + HALO, :]
                here = (lane >= 8 * q) & (lane < 8 * q + 8)
                west = jnp.where(here, pltpu.roll(part, 8 * q, 1) if q else part, west)
                east = jnp.where(here, pltpu.roll(part, 8 * q + 8, 1) if q < 15 else part, east)
            cpack[0, c, low : low + HALO, :] = reversed_eights(west)
            cpack[1, c, low : low + HALO, :] = reversed_eights(east)
        return carry

    def turn_right(c):
        right = [ext[c * PER + q, pl.ds(r, 8, stride=NR), :] for r in range(NR) for q in range(PER)]
        return jnp.concatenate(right, axis=0).astype(BF16)

    ends = jnp.concatenate([unit_one[0:8].astype(F32), unit_one[120:128].astype(F32)], axis=0).astype(BF16)

    def early_columns(c, carry):
        out = turned(ends, turn_right(c))
        for r in range(NR):
            eside[0, c, r] = out[0:8, 128 * r : 128 * r + 128]
            eside[1, c, r] = out[8:16, 128 * r : 128 * r + 128]
        for msg in column_messages(c):
            msg.start()
        return carry

    def put_corners(c):
        for side, at in ((0, 0), (1, HALO + COLS)):
            for r in range(NR):
                strip = xt[c, r, at : at + HALO, :]
                for which, row, b in ((side, r, 0), (2 + side, r - 2, 7)):
                    if 0 <= row < 8:
                        line = jnp.broadcast_to(corner[which, c, row : row + 1, :], (8, 128))
                        line = pltpu.roll(line, 0 if b else 121, 1, stride=1, stride_axis=0)
                        strip = jnp.where(block == b, line, strip)
                xt[c, r, at : at + HALO, :] = strip

    def state_messages(kind):
        wide, west, east = sext.at[kind], spk.at[kind, 0], spk.at[kind, 1]
        from_west, from_east = sst.at[kind, 0], sst.at[kind, 1]
        pairs = (
            (wide.at[:, pl.ds(HALO, HALO), :], wide.at[:, pl.ds(HALO + ROWS, HALO), :]),
            (wide.at[:, pl.ds(ROWS, HALO), :], wide.at[:, pl.ds(0, HALO), :]),
            (sthin.at[kind, 0], sland.at[kind, 1]),
            (sthin.at[kind, 1], sland.at[kind, 0]),
            (west.at[pl.ds(0, HALO), :], from_east.at[pl.ds(HALO + ROWS, HALO), :]),
            (east.at[pl.ds(0, HALO), :], from_west.at[pl.ds(HALO + ROWS, HALO), :]),
            (west.at[pl.ds(HALO, HALO), :], from_east.at[pl.ds(0, HALO), :]),
            (east.at[pl.ds(HALO, HALO), :], from_west.at[pl.ds(0, HALO), :]),
        )
        return [
            remote(src, dst, ssend.at[kind, way], srecv.at[kind, way], there(*WAYS[way]))
            for way, (src, dst) in enumerate(pairs)
        ]

    def share_state(kind):
        thin = [jnp.zeros((8, 128), F32)] * 2
        for k in range(8):
            at = HALO + 8 * k
            a = sext[kind, 0, at : at + 8, :]
            b = sext[kind, 1, at : at + 8, :]
            here = (lane >= 16 * k) & (lane < 16 * k + 8)
            both = (lane >= 16 * k) & (lane < 16 * k + 16)
            for side in range(2):
                first = (16 * k + 8 * side) % 128
                x = jnp.where(here, pltpu.roll(a, first, 1) if first else a, pltpu.roll(b, (first + 8) % 128, 1) if first != 120 else b)
                thin[side] = jnp.where(both, x, thin[side])
        for side in range(2):
            sthin[kind, side] = thin[side]
            spk[kind, side, 0:8, :] = thin[side]
            spk[kind, side, 8:16, :] = pltpu.roll(thin[side], 16, 1)
        msgs = state_messages(kind)
        for msg in msgs:
            msg.start()
        return msgs

    keep_north = jnp.where((gy == 0) & (block == 0), 0.0, 1.0)
    keep_south = jnp.where((gy == n_gy - 1) & (block == 7), 0.0, 1.0)
    keep_west = jnp.where((gx == 0) & (sub == 0), 0.0, 1.0)
    keep_east = jnp.where((gx == n_gx - 1) & (sub == 7), 0.0, 1.0)
    masks = (keep_north, keep_south, keep_west, keep_east)
    near_west = jnp.where((gx == 0) & (sub == 7), 0.0, 1.0)
    near_east = jnp.where((gx == n_gx - 1) & (sub == 0), 0.0, 1.0)

    def turn_state(kind):
        for side in range(2):
            thin = sland[kind, side]
            for k in range(8):
                sst[kind, side, HALO + 8 * k : 2 * HALO + 8 * k, :] = pltpu.roll(thin, 128 - 16 * k, 1) if k else thin
        west = by_rows(sst, kind, 0)
        east = by_rows(sst, kind, 1)
        levels = [by_rows(sext, kind, lev) for lev in range(LEVELS)]

        def keep(r, value):
            if r == 7:
                value = value * keep_north
            if r == 2:
                value = value * keep_south
            return value

        right = []
        for r in range(NR):
            right += [halves(jnp.concatenate([levels[0][r], levels[1][r]], axis=0))] * 8
        for base in (0, 8):
            both = []
            for lev in range(LEVELS):
                out = jnp.zeros((8, 128), F32)
                for r in range(base, min(base + 8, NR)):
                    at = 16 * (r - base)
                    w = west[r] if at == 8 * lev else pltpu.roll(west[r], (128 + at - 8 * lev) % 128, 1)
                    e = east[r] if at + 8 == 8 * lev else pltpu.roll(east[r], (128 + at + 8 - 8 * lev) % 128, 1)
                    out = jnp.where((lane >= at) & (lane < at + 8), w, out)
                    out = jnp.where((lane >= at + 8) & (lane < at + 16), e, out)
                both.append(out)
            right += [halves(jnp.concatenate(both, axis=0))] * 8
        out = turned(unit_two, jnp.concatenate(right, axis=0))
        for r in range(NR):
            for k in range(16):
                gt[r, HALO + 8 * k : HALO + 8 * k + 8, :] = keep(r, out[8 * k : 8 * k + 8, 128 * r : 128 * r + 128])
            at = 16 * (r % 8)
            side = slice(128 * (NR + r // 8), 128 * (NR + r // 8) + 128)
            gt[r, 0:8, :] = keep(r, out[at : at + 8, side] * near_west)
            gt[r, HALO + COLS : ECOLS, :] = keep(r, out[at + 8 : at + 16, side] * near_east)

    def turn_ensemble(c):
        for q in range(PER):
            f = c * PER + q
            ext[f, 0:HALO, :] = rhalo[f, 0:HALO, :]
            ext[f, HALO + ROWS : EROWS, :] = rhalo[f, HALO : 2 * HALO, :]
        out = turned(unit_one, turn_right(c))
        for r in range(NR):
            xt[c, r, HALO : HALO + COLS, :] = out[:, 128 * r : 128 * r + 128]

    def column(ref, t, *lead):
        return ref[(*lead, pl.ds(t, 8, stride=NT), slice(None))]

    def put_column(ref, t, value, *lead):
        ref[(*lead, pl.ds(t, 8, stride=NT), slice(None))] = value

    def apply(kind, c):
        def from_work(i):
            return lambda r, t: work[i, r, 8 * t : 8 * t + 8, :]

        def to_work(i):
            def store(r, t, value):
                work[i, r, 8 * t : 8 * t + 8, :] = value

            return store

        norms = {}

        def to_field(r, t, value):
            put_column(ft, t, value, kind, c, r)
            key = 3 * ((t >= 8) + (t >= 10)) + (r >= 2) + (r >= 8)
            norms[key] = norms[key] + value * value if key in norms else value * value

        def to_image(r, t, value):
            put_column(acc, t, column(acc, t, r) + value * column(xt, t, c, r), r)

        sweep(lambda r, t: column(xt, t, c, r) * column(gt, t, r), to_work(0), masks)
        sweep(from_work(0), to_work(1), masks)
        sweep(from_work(1), to_work(0), masks)
        sweep(from_work(0), to_field, masks)
        for key, value in norms.items():
            squares[kind, key] += value
        sweep(lambda r, t: column(ft, t, kind, c, r), to_work(1), masks)
        sweep(from_work(1), to_work(0), masks)
        sweep(from_work(0), to_work(1), masks)
        sweep(from_work(1), to_image, masks)

    def state_image(kind):
        for r in range(NR):
            out = turned(members, halves(acc[r, HALO : HALO + COLS, :])) * FILTER_SCALE
            for lev in range(LEVELS):
                image[kind, lev, pl.ds(r, 8, stride=NR), :] = out[8 * lev : 8 * lev + 8]

    def turn_back(kind, chunks):
        out_ref = (base_out, grown_out)[kind]

        def one(i, carry):
            c = i // NR
            r = lax.rem(i, NR)
            out = turned(unit_two, halves(ft[kind, c, r, HALO : HALO + COLS, :]))
            for q in range(PER):
                out_ref[c * PER + q, pl.ds(r, 8, stride=NR), :] = out[8 * q : 8 * q + 8]
            return carry

        lax.fori_loop(chunks[0] * NR, chunks[1] * NR, one, 0, unroll=5)

    pl.semaphore_wait(barrier, len(met))
    for msg in row_messages(0):
        msg.start()
    smsgs = share_state(0)
    widen(1)
    widen(2)
    widen(3)
    lax.fori_loop(0, CHUNKS, pack_corners, 0)
    for msg in corner_messages():
        msg.start()
    lax.fori_loop(0, CHUNKS, early_columns, 0)
    for msg in row_messages(1):
        msg.start()
    for msg in row_messages(2):
        msg.start()
    for msg in row_messages(3):
        msg.start()
    squares[...] = jnp.zeros_like(squares)
    acc[...] = jnp.zeros_like(acc)

    for msg in smsgs:
        msg.wait_recv()
    turn_state(0)
    for msg in corner_messages():
        msg.wait_recv()

    def first_pass(c, carry):
        for msg in column_messages(c):
            msg.wait_recv()
        put_corners(c)
        for msg in row_messages(c):
            msg.wait_recv()
        turn_ensemble(c)
        apply(0, c)
        return carry

    lax.fori_loop(0, CHUNKS, first_pass, 0)
    state_image(0)

    for lev in range(LEVELS):
        inner = slice(HALO, HALO + ROWS)
        sext[1, lev, inner, :] = image[0, lev, inner, :] * dext[lev, inner, :] * FILTER_SCALE
    vmsgs = share_state(1)
    acc[...] = jnp.zeros_like(acc)
    turn_back(0, (0, 2))
    for msg in vmsgs:
        msg.wait_recv()
    turn_state(1)

    def second_pass(c, carry):
        apply(1, c)
        return carry

    lax.fori_loop(0, CHUNKS, second_pass, 0)
    state_image(1)

    def norm(kind):
        parts = []
        for key in range(9):
            inside = None
            for test in (
                [sub > 0] if key // 3 == 0 else [sub < 7] if key // 3 == 2 else []
            ) + ([block > 0] if key % 3 < 2 else []) + ([block < 7] if key % 3 > 0 else []):
                inside = test if inside is None else inside & test
            parts.append(jnp.where(inside, squares[kind, key], 0.0))
        return jnp.sum(total(parts))

    def weighted(kind):
        parts = []
        for lev in range(LEVELS):
            for k in range(ROWS // 8):
                at = slice(HALO + 8 * k, HALO + 8 * k + 8)
                parts.append(dext[lev, at, :] * (image[kind, lev, at, :] * image[kind, lev, at, :]))
        return jnp.sum(total(parts))

    mine = (norm(0), weighted(0), norm(1), weighted(1))
    line = lane[0:1]
    row = jnp.where(line < 64, jnp.where(line < 32, mine[0], mine[1]), jnp.where(line < 96, mine[2], mine[3]))

    def gather(value, ref, me, n, send, recv, to, fill):
        ref[me] = value
        copies = [remote(ref.at[me], ref.at[me], send.at[k], recv.at[k], to(k)) for k in range(1, n)]
        for copy in copies:
            copy.start()
        for kind, chunks in fill:
            turn_back(kind, chunks)
        for copy in copies:
            copy.wait_recv()
        return copies, jnp.sum(ref[...], axis=0)

    acopies, row = gather(row, rowa, gx, n_gx, asend, arecv, lambda k: there(0, k), [(0, (2, 4))])
    bcopies, row = gather(row, rowb, gy, n_gy, bsend, brecv, lambda k: there(k, 0), [(1, (0, 4))])

    sums = [jnp.full((8, 128), jnp.sum(jnp.where(line == 32 * i, row, 0.0)), F32) for i in range(4)]
    bnorm_sq = sums[0] + EPS
    bnorm = jnp.sqrt(bnorm_sq)
    unit, cross, square, cube = [s / bnorm_sq for s in sums]
    alpha_one = unit + cross
    shift = 1.0 - alpha_one
    remain_sq = jnp.maximum(shift * shift * unit + 2.0 * shift * cross + square, 0.0)
    beta_sq = remain_sq + EPS
    beta = jnp.sqrt(beta_sq)
    curve = jnp.maximum(shift * shift * cross + 2.0 * shift * square + cube, 0.0)
    alpha_two = (remain_sq + curve) / beta_sq
    determ = alpha_one * alpha_two - beta_sq
    coef_one = bnorm * alpha_two / determ
    coef_two = -bnorm * beta / determ
    on_base = coef_one / bnorm + coef_two * shift / (bnorm * beta)
    on_grown = coef_two / (bnorm * beta)

    coef[0] = on_base
    coef[1] = on_grown
    for c in range(CHUNKS):
        for msg in row_messages(c) + column_messages(c):
            msg.wait_send()
    for msg in corner_messages() + smsgs + vmsgs + acopies + bcopies:
        msg.wait_send()


def combine(base, grown, image, coef, control, increment, staged, small, out_sem):
    a, b = coef[0], coef[1]
    copies = []
    for i in range(BATCHES):

        def one(k, carry):
            f = i * BATCH + k
            for r in range(ROWS // 8):
                at = slice(HALO + 8 * r, HALO + 8 * r + 8)
                staged[f, 8 * r : 8 * r + 8, :] = a * base[f, at, :] + b * grown[f, at, :]
            return carry

        lax.fori_loop(0, BATCH, one, 0, unroll=2)
        part = pl.ds(i * BATCH, BATCH)
        copies.append(pltpu.make_async_copy(staged.at[part], control.at[part], out_sem.at[i]))
        copies[-1].start()
    for lev in range(LEVELS):
        for r in range(ROWS // 8):
            at = slice(HALO + 8 * r, HALO + 8 * r + 8)
            small[lev, 8 * r : 8 * r + 8, :] = a * image[0, lev, at, :] + b * image[1, lev, at, :]
    copies.append(pltpu.make_async_copy(small, increment, out_sem.at[BATCHES]))
    copies[-1].start()
    for copy in copies:
        copy.wait()


def solution(mesh):
    n_gy, n_gx = mesh.shape["gy"], mesh.shape["gx"]

    def on_device(ensemble, obs_cell, obs_level, innovation, obs_weight):
        obs = obs_cell.shape[-1]
        fields = MEMBERS * LEVELS
        vmem = pltpu.VMEM
        dma = pltpu.SemaphoreType.DMA
        base, grown, image, coef = pl.pallas_call(
            lambda *refs: kernel(n_gy, n_gx, *refs),
            name="lanczos",
            out_shape=(
                jax.ShapeDtypeStruct((fields, EROWS, COLS), F32),
                jax.ShapeDtypeStruct((fields, EROWS, COLS), F32),
                jax.ShapeDtypeStruct((2, LEVELS, EROWS, COLS), F32),
                jax.ShapeDtypeStruct((2, 8, COLS), F32),
            ),
            in_specs=[pl.BlockSpec(memory_space=pltpu.HBM)] * 5,
            out_specs=(pl.BlockSpec(memory_space=vmem),) * 4,
            scratch_shapes=[
                vmem((fields, ROWS, COLS), BF16),
                vmem((1, 1, obs), jnp.int32),
                vmem((1, 1, obs), jnp.int32),
                vmem((1, 1, obs), F32),
                vmem((1, 1, obs), F32),
                vmem((fields, EROWS, COLS), F32),
                vmem((fields, 2 * HALO, COLS), F32),
                vmem((2, CHUNKS, NR, HALO, 128), F32),
                vmem((2, CHUNKS, 2 * HALO, 128), F32),
                vmem((4, CHUNKS, HALO, 128), F32),
                vmem((CHUNKS, NR, ECOLS, 128), F32),
                vmem((NR, ECOLS, 128), F32),
                vmem((2, LEVELS, EROWS, COLS), F32),
                vmem((2, 2, 2 * HALO, COLS), F32),
                vmem((2, 2, HALO, COLS), F32),
                vmem((2, 2, HALO, COLS), F32),
                vmem((2, 2, EROWS, COLS), F32),
                vmem((LEVELS, EROWS, COLS), F32),
                vmem((4 * ROWS, LEVELS * COLS), F32),
                vmem((2, NR, ECOLS, 128), F32),
                vmem((2, CHUNKS, NR, ECOLS, 128), F32),
                vmem((NR, ECOLS, 128), F32),
                vmem((2, 9, 8, 128), F32),
                vmem((n_gx, 1, COLS), F32),
                vmem((n_gy, 1, COLS), F32),
                dma((CHUNKS + 4,)),
                dma((CHUNKS, 4)),
                dma((CHUNKS, 4)),
                dma((4,)),
                dma((4,)),
                dma((2, 8)),
                dma((2, 8)),
                dma((n_gx,)),
                dma((n_gx,)),
                dma((n_gy,)),
                dma((n_gy,)),
            ],
            compiler_params=pltpu.CompilerParams(
                collective_id=0, has_side_effects=True, vmem_limit_bytes=28 * 1024 * 1024
            ),
        )(
            *[
                pltpu.with_memory_space_constraint(x, pltpu.HBM)
                for x in (ensemble.reshape(fields, ROWS, COLS), obs_cell, obs_level, innovation, obs_weight)
            ]
        )
        control, increment = pl.pallas_call(
            combine,
            name="combine",
            out_shape=(
                jax.ShapeDtypeStruct((fields, ROWS, COLS), F32),
                jax.ShapeDtypeStruct((LEVELS, ROWS, COLS), F32),
            ),
            in_specs=[pl.BlockSpec(memory_space=vmem)] * 4,
            out_specs=(pl.BlockSpec(memory_space=pltpu.HBM),) * 2,
            scratch_shapes=[
                vmem((fields, ROWS, COLS), F32),
                vmem((LEVELS, ROWS, COLS), F32),
                dma((BATCHES + 1,)),
            ],
            compiler_params=pltpu.CompilerParams(vmem_limit_bytes=12 * 1024 * 1024),
        )(base, grown, image, coef)
        return control.reshape(MEMBERS, LEVELS, ROWS, COLS), increment

    return jax.shard_map(
        on_device,
        mesh=mesh,
        in_specs=(P(None, None, "gy", "gx"),) + (P("gy", "gx", None),) * 4,
        out_specs=(P(None, None, "gy", "gx"), P(None, "gy", "gx")),
        check_vma=False,
    )
```

```python
import jax
import jax.numpy as jnp
from jax import lax
from jax.experimental import pallas as pl
from jax.experimental.pallas import tpu as pltpu
from jax.sharding import PartitionSpec as P

MESH = pl.DeviceIdType.MESH
F32 = jnp.float32
BF16 = jnp.bfloat16
EPS = 1e-06
FILTER_SCALE = 0.2**4
MEMBERS = 32
LEVELS = 2
ROWS = 64
COLS = 128
HALO = 8
EROWS = ROWS + 2 * HALO
ECOLS = COLS + 2 * HALO
NR = EROWS // 8
NT = ECOLS // 8
CHUNKS = 4
PER = 16
OBS_STEP = 512
BATCHES = 8
BATCH = MEMBERS * LEVELS // BATCHES

WAYS = ((-1, 0), (1, 0), (0, -1), (0, 1), (-1, -1), (-1, 1), (1, -1), (1, 1))


def total(values):
    while len(values) > 1:
        odd = values[len(values) - len(values) % 2 :]
        values = [a + b for a, b in zip(values[0::2], values[1::2])] + odd
    return values[0]


def by_rows(ref, *lead):
    return [ref[(*lead, pl.ds(r, 8, stride=NR), slice(None))] for r in range(NR)]


def put_rows(ref, values, *lead):
    for r in range(NR):
        ref[(*lead, pl.ds(r, 8, stride=NR), slice(None))] = values[r]


def tiles(ref, *lead):
    return [ref[(*lead, slice(8 * r, 8 * r + 8), slice(None))] for r in range(NR)]


def put_tiles(ref, values, *lead):
    for r in range(NR):
        ref[(*lead, slice(8 * r, 8 * r + 8), slice(None))] = values[r]


def halves(x):
    high = x.astype(BF16)
    return jnp.concatenate([high, (x - high.astype(F32)).astype(BF16)], axis=1)


def turned(left, right):
    return lax.dot_general(left, right, (((1,), (1,)), ((), ())), preferred_element_type=F32)


def sweep(load, store, masks):
    north, south, west, east = masks or (None,) * 4
    for first, last in ((0, NT // 2), (NT // 2, NT)):
        seen = {}

        def f(r, t):
            if (r, t) not in seen:
                if t == -1:
                    value = pltpu.roll(f(r, NT - 1), 1, 0)
                elif t == NT:
                    value = pltpu.roll(f(r, 0), 7, 0)
                elif r == -1:
                    value = pltpu.roll(f(NR - 1, t), 1, 1)
                elif r == NR:
                    value = pltpu.roll(f(0, t), 127, 1)
                else:
                    value = load(r, t)
                seen[r, t] = value
            return seen[r, t]

        def pair_row(r):
            return {t: f(r, t) + f(r + 1, t - 1) for t in range(first, last + 1)}

        def finish(r, above, here):
            for t in range(first, last):
                out = f(r, t) + (above[t] + here[t + 1])
                if masks and r == 7:
                    out = out * north
                if masks and r == 2:
                    out = out * south
                if masks and t == 7:
                    out = out * west
                if masks and t == 10:
                    out = out * east
                store(r, t, out)

        start = above = pair_row(0)
        for r in range(1, NR):
            here = pair_row(r)
            finish(r, above, here)
            above = here
        finish(0, pair_row(-1), start)


def kernel(
    n_gy,
    n_gx,
    ens,
    cell,
    level,
    innov,
    weight,
    base_out,
    grown_out,
    image,
    coef,
    xin,
    cin,
    lin,
    iin,
    win,
    ext,
    rhalo,
    eside,
    cpack,
    corner,
    xt,
    gt,
    sext,
    spk,
    sthin,
    sland,
    sst,
    dext,
    grid,
    work,
    ft,
    acc,
    squares,
    rowa,
    rowb,
    in_sem,
    xsend,
    xrecv,
    csend,
    crecv,
    ssend,
    srecv,
    asend,
    arecv,
    bsend,
    brecv,
):
    gy = lax.axis_index("gy")
    gx = lax.axis_index("gx")
    lane = lax.broadcasted_iota(jnp.int32, (8, 128), 1)
    sub = lax.broadcasted_iota(jnp.int32, (8, 128), 0)
    block = lane & 7
    down = lax.broadcasted_iota(jnp.int32, (128, 128), 0)
    across = lax.broadcasted_iota(jnp.int32, (128, 128), 1)
    unit_one = jnp.where(down == across, 1.0, 0.0).astype(BF16)
    unit_two = jnp.concatenate([unit_one, unit_one], axis=1)
    members = jnp.where(down[:16] == (across[:16] & 15), 1.0, 0.0).astype(BF16)
    members = jnp.concatenate([members, members], axis=1)

    loads = [
        pltpu.make_async_copy(src, dst, in_sem.at[i])
        for i, (src, dst) in enumerate(
            [(ens.at[pl.ds(c * PER, PER)], xin.at[pl.ds(c * PER, PER)]) for c in range(CHUNKS)]
            + [(cell, cin), (level, lin), (innov, iin), (weight, win)]
        )
    ]
    for load in loads:
        load.start()

    def there(dy, dx):
        return (lax.rem(gy + dy + n_gy, n_gy), lax.rem(gx + dx + n_gx, n_gx))

    def remote(src, dst, send, recv, to):
        return pltpu.make_async_remote_copy(
            src_ref=src, dst_ref=dst, send_sem=send, recv_sem=recv, device_id=to, device_id_type=MESH
        )

    barrier = pltpu.get_barrier_semaphore()
    met = [(0, k) for k in range(1, n_gx)] + [(k, 0) for k in range(1, n_gy)] + list(WAYS[4:])
    for dy, dx in met:
        pl.semaphore_signal(barrier, inc=1, device_id=there(dy, dx), device_id_type=MESH)

    for load in loads[CHUNKS:]:
        load.wait()
    grid[...] = jnp.zeros_like(grid)

    def scatter(k, carry):
        part = pl.ds(pl.multiple_of(k * OBS_STEP, OBS_STEP), OBS_STEP)
        where_at = cin[0, :, part]
        row = where_at >> 7
        col = (where_at & 127) + lin[0, :, part] * COLS
        w = win[0, :, part]
        on_row = lax.broadcasted_iota(jnp.int32, (ROWS, OBS_STEP), 0) == row
        on_col = lax.broadcasted_iota(jnp.int32, (LEVELS * COLS, OBS_STEP), 0) == col
        right = jnp.where(on_col, 1.0, 0.0).astype(BF16)
        left = []
        for value in (w * iin[0, :, part], w):
            for _ in range(2):
                piece = value.astype(BF16).astype(F32)
                left.append(jnp.where(on_row, piece, 0.0).astype(BF16))
                value = value - piece
        left = jnp.concatenate(left, axis=0)
        grid[...] += lax.dot_general(left, right, (((1,), (1,)), ((), ())), preferred_element_type=F32)
        return carry

    lax.fori_loop(0, cin.shape[-1] // OBS_STEP, scatter, 0)
    for lev in range(LEVELS):
        cols = slice(lev * COLS, lev * COLS + COLS)
        grad = grid[0:64, cols] + grid[64:128, cols]
        diag = grid[128:192, cols] + grid[192:256, cols]
        sext[0, lev, HALO : HALO + ROWS, :] = grad * FILTER_SCALE
        dext[lev, 0:HALO, :] = jnp.zeros((HALO, COLS), F32)
        dext[lev, HALO : HALO + ROWS, :] = diag
        dext[lev, HALO + ROWS : EROWS, :] = jnp.zeros((HALO, COLS), F32)

    def widen(c):
        loads[c].wait()

        def one(i, carry):
            for k in range(4):
                f = c * PER + 4 * i + k
                ext[f, 0:HALO, :] = jnp.zeros((HALO, COLS), F32)
                ext[f, HALO + ROWS : EROWS, :] = jnp.zeros((HALO, COLS), F32)
                ext[f, HALO : HALO + ROWS, :] = xin[f].astype(F32)
            return carry

        lax.fori_loop(0, PER // 4, one, 0)

    widen(0)

    def row_messages(c):
        fields = pl.ds(c * PER, PER)
        return [
            remote(ext.at[fields, pl.ds(src, HALO), :], rhalo.at[fields, pl.ds(dst, HALO), :], xsend.at[c, way], xrecv.at[c, way], there(*WAYS[way]))
            for way, (src, dst) in enumerate(((HALO, HALO), (ROWS, 0)))
        ]

    def column_messages(c):
        return [
            remote(eside.at[side, c], xt.at[c, :, pl.ds(dst, HALO), :], xsend.at[c, 2 + side], xrecv.at[c, 2 + side], there(*WAYS[2 + side]))
            for side, dst in ((0, HALO + COLS), (1, 0))
        ]

    def corner_messages():
        return [
            remote(cpack.at[side, :, pl.ds(low, HALO), :], corner.at[3 - k], csend.at[k], crecv.at[k], there(*WAYS[4 + k]))
            for k, (side, low) in enumerate(((0, 0), (1, 0), (0, HALO), (1, HALO)))
        ]

    def reversed_eights(x):
        for width in (1, 2, 4):
            x = jnp.where((lane & width) == 0, pltpu.roll(x, 128 - width, 1), pltpu.roll(x, width, 1))
        return x

    def pack_corners(c, carry):
        for low, at in ((0, HALO), (HALO, ROWS)):
            west = jnp.zeros((8, 128), F32)
            east = jnp.zeros((8, 128), F32)
            for q in range(PER):
                part = ext[c * PER + q, at : at + HALO, :]
                here = (lane >= 8 * q) & (lane < 8 * q + 8)
                west = jnp.where(here, pltpu.roll(part, 8 * q, 1) if q else part, west)
                east = jnp.where(here, pltpu.roll(part, 8 * q + 8, 1) if q < 15 else part, east)
            cpack[0, c, low : low + HALO, :] = reversed_eights(west)
            cpack[1, c, low : low + HALO, :] = reversed_eights(east)
        return carry

    def turn_right(c):
        right = [ext[c * PER + q, pl.ds(r, 8, stride=NR), :] for r in range(NR) for q in range(PER)]
        return jnp.concatenate(right, axis=0).astype(BF16)

    ends = jnp.concatenate([unit_one[0:8].astype(F32), unit_one[120:128].astype(F32)], axis=0).astype(BF16)

    def early_columns(c, carry):
        out = turned(ends, turn_right(c))
        for r in range(NR):
            eside[0, c, r] = out[0:8, 128 * r : 128 * r + 128]
            eside[1, c, r] = out[8:16, 128 * r : 128 * r + 128]
        for msg in column_messages(c):
            msg.start()
        return carry

    def put_corners(c):
        for side, at in ((0, 0), (1, HALO + COLS)):
            for r in range(NR):
                strip = xt[c, r, at : at + HALO, :]
                for which, row, b in ((side, r, 0), (2 + side, r - 2, 7)):
                    if 0 <= row < 8:
                        line = jnp.broadcast_to(corner[which, c, row : row + 1, :], (8, 128))
                        line = pltpu.roll(line, 0 if b else 121, 1, stride=1, stride_axis=0)
                        strip = jnp.where(block == b, line, strip)
                xt[c, r, at : at + HALO, :] = strip

    def state_messages(kind):
        wide, west, east = sext.at[kind], spk.at[kind, 0], spk.at[kind, 1]
        from_west, from_east = sst.at[kind, 0], sst.at[kind, 1]
        pairs = (
            (wide.at[:, pl.ds(HALO, HALO), :], wide.at[:, pl.ds(HALO + ROWS, HALO), :]),
            (wide.at[:, pl.ds(ROWS, HALO), :], wide.at[:, pl.ds(0, HALO), :]),
            (sthin.at[kind, 0], sland.at[kind, 1]),
            (sthin.at[kind, 1], sland.at[kind, 0]),
            (west.at[pl.ds(0, HALO), :], from_east.at[pl.ds(HALO + ROWS, HALO), :]),
            (east.at[pl.ds(0, HALO), :], from_west.at[pl.ds(HALO + ROWS, HALO), :]),
            (west.at[pl.ds(HALO, HALO), :], from_east.at[pl.ds(0, HALO), :]),
            (east.at[pl.ds(HALO, HALO), :], from_west.at[pl.ds(0, HALO), :]),
        )
        return [
            remote(src, dst, ssend.at[kind, way], srecv.at[kind, way], there(*WAYS[way]))
            for way, (src, dst) in enumerate(pairs)
        ]

    def share_state(kind):
        thin = [jnp.zeros((8, 128), F32)] * 2
        for k in range(8):
            at = HALO + 8 * k
            a = sext[kind, 0, at : at + 8, :]
            b = sext[kind, 1, at : at + 8, :]
            here = (lane >= 16 * k) & (lane < 16 * k + 8)
            both = (lane >= 16 * k) & (lane < 16 * k + 16)
            for side in range(2):
                first = (16 * k + 8 * side) % 128
                x = jnp.where(here, pltpu.roll(a, first, 1) if first else a, pltpu.roll(b, (first + 8) % 128, 1) if first != 120 else b)
                thin[side] = jnp.where(both, x, thin[side])
        for side in range(2):
            sthin[kind, side] = thin[side]
            spk[kind, side, 0:8, :] = thin[side]
            spk[kind, side, 8:16, :] = pltpu.roll(thin[side], 16, 1)
        msgs = state_messages(kind)
        for msg in msgs:
            msg.start()
        return msgs

    keep_north = jnp.where((gy == 0) & (block == 0), 0.0, 1.0)
    keep_south = jnp.where((gy == n_gy - 1) & (block == 7), 0.0, 1.0)
    keep_west = jnp.where((gx == 0) & (sub == 0), 0.0, 1.0)
    keep_east = jnp.where((gx == n_gx - 1) & (sub == 7), 0.0, 1.0)
    masks = (keep_north, keep_south, keep_west, keep_east)
    near_west = jnp.where((gx == 0) & (sub == 7), 0.0, 1.0)
    near_east = jnp.where((gx == n_gx - 1) & (sub == 0), 0.0, 1.0)

    def turn_state(kind):
        for side in range(2):
            thin = sland[kind, side]
            for k in range(8):
                sst[kind, side, HALO + 8 * k : 2 * HALO + 8 * k, :] = pltpu.roll(thin, 128 - 16 * k, 1) if k else thin
        west = by_rows(sst, kind, 0)
        east = by_rows(sst, kind, 1)
        levels = [by_rows(sext, kind, lev) for lev in range(LEVELS)]

        def keep(r, value):
            if r == 7:
                value = value * keep_north
            if r == 2:
                value = value * keep_south
            return value

        right = []
        for r in range(NR):
            right += [halves(jnp.concatenate([levels[0][r], levels[1][r]], axis=0))] * 8
        for base in (0, 8):
            both = []
            for lev in range(LEVELS):
                out = jnp.zeros((8, 128), F32)
                for r in range(base, min(base + 8, NR)):
                    at = 16 * (r - base)
                    w = west[r] if at == 8 * lev else pltpu.roll(west[r], (128 + at - 8 * lev) % 128, 1)
                    e = east[r] if at + 8 == 8 * lev else pltpu.roll(east[r], (128 + at + 8 - 8 * lev) % 128, 1)
                    out = jnp.where((lane >= at) & (lane < at + 8), w, out)
                    out = jnp.where((lane >= at + 8) & (lane < at + 16), e, out)
                both.append(out)
            right += [halves(jnp.concatenate(both, axis=0))] * 8
        out = turned(unit_two, jnp.concatenate(right, axis=0))
        for r in range(NR):
            for k in range(16):
                gt[r, HALO + 8 * k : HALO + 8 * k + 8, :] = keep(r, out[8 * k : 8 * k + 8, 128 * r : 128 * r + 128])
            at = 16 * (r % 8)
            side = slice(128 * (NR + r // 8), 128 * (NR + r // 8) + 128)
            gt[r, 0:8, :] = keep(r, out[at : at + 8, side] * near_west)
            gt[r, HALO + COLS : ECOLS, :] = keep(r, out[at + 8 : at + 16, side] * near_east)

    def turn_ensemble(c):
        for q in range(PER):
            f = c * PER + q
            ext[f, 0:HALO, :] = rhalo[f, 0:HALO, :]
            ext[f, HALO + ROWS : EROWS, :] = rhalo[f, HALO : 2 * HALO, :]
        out = turned(unit_one, turn_right(c))
        for r in range(NR):
            xt[c, r, HALO : HALO + COLS, :] = out[:, 128 * r : 128 * r + 128]

    def column(ref, t, *lead):
        return ref[(*lead, pl.ds(t, 8, stride=NT), slice(None))]

    def put_column(ref, t, value, *lead):
        ref[(*lead, pl.ds(t, 8, stride=NT), slice(None))] = value

    def apply(kind, c):
        def from_work(i):
            return lambda r, t: work[i, r, 8 * t : 8 * t + 8, :]

        def to_work(i):
            def store(r, t, value):
                work[i, r, 8 * t : 8 * t + 8, :] = value

            return store

        norms = {}

        def to_field(r, t, value):
            put_column(ft, t, value, kind, c, r)
            key = 3 * ((t >= 8) + (t >= 10)) + (r >= 2) + (r >= 8)
            norms[key] = norms[key] + value * value if key in norms else value * value

        def to_image(r, t, value):
            put_column(acc, t, column(acc, t, r) + value * column(xt, t, c, r), r)

        sweep(lambda r, t: column(xt, t, c, r) * column(gt, t, r), to_work(0), masks)
        sweep(from_work(0), to_work(1), masks)
        sweep(from_work(1), to_work(0), masks)
        sweep(from_work(0), to_field, masks)
        for key, value in norms.items():
            squares[kind, key] += value
        sweep(lambda r, t: column(ft, t, kind, c, r), to_work(1), masks)
        sweep(from_work(1), to_work(0), masks)
        sweep(from_work(0), to_work(1), masks)
        sweep(from_work(1), to_image, None)

    def state_image(kind):
        for r in range(NR):
            out = turned(members, halves(acc[r, HALO : HALO + COLS, :])) * FILTER_SCALE
            for lev in range(LEVELS):
                image[kind, lev, pl.ds(r, 8, stride=NR), :] = out[8 * lev : 8 * lev + 8]

    def turn_back(kind, chunks):
        out_ref = (base_out, grown_out)[kind]

        def one(i, carry):
            c = i // NR
            r = lax.rem(i, NR)
            out = turned(unit_two, halves(ft[kind, c, r, HALO : HALO + COLS, :]))
            for q in range(PER):
                out_ref[c * PER + q, pl.ds(r, 8, stride=NR), :] = out[8 * q : 8 * q + 8]
            return carry

        lax.fori_loop(chunks[0] * NR, chunks[1] * NR, one, 0, unroll=5)

    pl.semaphore_wait(barrier, len(met))
    for msg in row_messages(0):
        msg.start()
    smsgs = share_state(0)
    widen(1)
    widen(2)
    widen(3)
    lax.fori_loop(0, CHUNKS, pack_corners, 0)
    for msg in corner_messages():
        msg.start()
    lax.fori_loop(0, CHUNKS, early_columns, 0)
    for msg in row_messages(1):
        msg.start()
    for msg in row_messages(2):
        msg.start()
    for msg in row_messages(3):
        msg.start()
    squares[...] = jnp.zeros_like(squares)
    acc[...] = jnp.zeros_like(acc)

    for msg in smsgs:
        msg.wait_recv()
    turn_state(0)
    for msg in corner_messages():
        msg.wait_recv()

    def first_pass(c, carry):
        for msg in column_messages(c):
            msg.wait_recv()
        put_corners(c)
        for msg in row_messages(c):
            msg.wait_recv()
        turn_ensemble(c)
        apply(0, c)
        return carry

    lax.fori_loop(0, CHUNKS, first_pass, 0)
    state_image(0)

    for lev in range(LEVELS):
        inner = slice(HALO, HALO + ROWS)
        sext[1, lev, inner, :] = image[0, lev, inner, :] * dext[lev, inner, :] * FILTER_SCALE
    vmsgs = share_state(1)
    acc[...] = jnp.zeros_like(acc)
    turn_back(0, (0, 2))
    for msg in vmsgs:
        msg.wait_recv()
    turn_state(1)

    def second_pass(c, carry):
        apply(1, c)
        return carry

    lax.fori_loop(0, CHUNKS, second_pass, 0)
    state_image(1)

    def norm(kind):
        parts = []
        for key in range(9):
            inside = None
            for test in (
                [sub > 0] if key // 3 == 0 else [sub < 7] if key // 3 == 2 else []
            ) + ([block > 0] if key % 3 < 2 else []) + ([block < 7] if key % 3 > 0 else []):
                inside = test if inside is None else inside & test
            parts.append(jnp.where(inside, squares[kind, key], 0.0))
        return jnp.sum(total(parts))

    def weighted(kind):
        parts = []
        for lev in range(LEVELS):
            for k in range(ROWS // 8):
                at = slice(HALO + 8 * k, HALO + 8 * k + 8)
                parts.append(dext[lev, at, :] * (image[kind, lev, at, :] * image[kind, lev, at, :]))
        return jnp.sum(total(parts))

    mine = (norm(0), weighted(0), norm(1), weighted(1))
    line = lane[0:1]
    row = jnp.where(line < 64, jnp.where(line < 32, mine[0], mine[1]), jnp.where(line < 96, mine[2], mine[3]))

    def gather(value, ref, me, n, send, recv, to, fill):
        ref[me] = value
        copies = [remote(ref.at[me], ref.at[me], send.at[k], recv.at[k], to(k)) for k in range(1, n)]
        for copy in copies:
            copy.start()
        for kind, chunks in fill:
            turn_back(kind, chunks)
        for copy in copies:
            copy.wait_recv()
        return copies, jnp.sum(ref[...], axis=0)

    acopies, row = gather(row, rowa, gx, n_gx, asend, arecv, lambda k: there(0, k), [(0, (2, 4))])
    bcopies, row = gather(row, rowb, gy, n_gy, bsend, brecv, lambda k: there(k, 0), [(1, (0, 4))])

    sums = [jnp.full((8, 128), jnp.sum(jnp.where(line == 32 * i, row, 0.0)), F32) for i in range(4)]
    bnorm_sq = sums[0] + EPS
    bnorm = jnp.sqrt(bnorm_sq)
    unit, cross, square, cube = [s / bnorm_sq for s in sums]
    alpha_one = unit + cross
    shift = 1.0 - alpha_one
    remain_sq = jnp.maximum(shift * shift * unit + 2.0 * shift * cross + square, 0.0)
    beta_sq = remain_sq + EPS
    beta = jnp.sqrt(beta_sq)
    curve = jnp.maximum(shift * shift * cross + 2.0 * shift * square + cube, 0.0)
    alpha_two = (remain_sq + curve) / beta_sq
    determ = alpha_one * alpha_two - beta_sq
    coef_one = bnorm * alpha_two / determ
    coef_two = -bnorm * beta / determ
    on_base = coef_one / bnorm + coef_two * shift / (bnorm * beta)
    on_grown = coef_two / (bnorm * beta)

    coef[0] = on_base
    coef[1] = on_grown
    for c in range(CHUNKS):
        for msg in row_messages(c) + column_messages(c):
            msg.wait_send()
    for msg in corner_messages() + smsgs + vmsgs + acopies + bcopies:
        msg.wait_send()


def combine(base, grown, image, coef, control, increment, staged, small, out_sem):
    a, b = coef[0], coef[1]
    copies = []
    for i in range(BATCHES):

        def one(k, carry):
            f = i * BATCH + k
            for r in range(ROWS // 8):
                at = slice(HALO + 8 * r, HALO + 8 * r + 8)
                staged[f, 8 * r : 8 * r + 8, :] = a * base[f, at, :] + b * grown[f, at, :]
            return carry

        lax.fori_loop(0, BATCH, one, 0, unroll=2)
        part = pl.ds(i * BATCH, BATCH)
        copies.append(pltpu.make_async_copy(staged.at[part], control.at[part], out_sem.at[i]))
        copies[-1].start()
    for lev in range(LEVELS):
        for r in range(ROWS // 8):
            at = slice(HALO + 8 * r, HALO + 8 * r + 8)
            small[lev, 8 * r : 8 * r + 8, :] = a * image[0, lev, at, :] + b * image[1, lev, at, :]
    copies.append(pltpu.make_async_copy(small, increment, out_sem.at[BATCHES]))
    copies[-1].start()
    for copy in copies:
        copy.wait()


def solution(mesh):
    n_gy, n_gx = mesh.shape["gy"], mesh.shape["gx"]

    def on_device(ensemble, obs_cell, obs_level, innovation, obs_weight):
        obs = obs_cell.shape[-1]
        fields = MEMBERS * LEVELS
        vmem = pltpu.VMEM
        dma = pltpu.SemaphoreType.DMA
        base, grown, image, coef = pl.pallas_call(
            lambda *refs: kernel(n_gy, n_gx, *refs),
            name="lanczos",
            out_shape=(
                jax.ShapeDtypeStruct((fields, EROWS, COLS), F32),
                jax.ShapeDtypeStruct((fields, EROWS, COLS), F32),
                jax.ShapeDtypeStruct((2, LEVELS, EROWS, COLS), F32),
                jax.ShapeDtypeStruct((2, 8, COLS), F32),
            ),
            in_specs=[pl.BlockSpec(memory_space=pltpu.HBM)] * 5,
            out_specs=(pl.BlockSpec(memory_space=vmem),) * 4,
            scratch_shapes=[
                vmem((fields, ROWS, COLS), BF16),
                vmem((1, 1, obs), jnp.int32),
                vmem((1, 1, obs), jnp.int32),
                vmem((1, 1, obs), F32),
                vmem((1, 1, obs), F32),
                vmem((fields, EROWS, COLS), F32),
                vmem((fields, 2 * HALO, COLS), F32),
                vmem((2, CHUNKS, NR, HALO, 128), F32),
                vmem((2, CHUNKS, 2 * HALO, 128), F32),
                vmem((4, CHUNKS, HALO, 128), F32),
                vmem((CHUNKS, NR, ECOLS, 128), F32),
                vmem((NR, ECOLS, 128), F32),
                vmem((2, LEVELS, EROWS, COLS), F32),
                vmem((2, 2, 2 * HALO, COLS), F32),
                vmem((2, 2, HALO, COLS), F32),
                vmem((2, 2, HALO, COLS), F32),
                vmem((2, 2, EROWS, COLS), F32),
                vmem((LEVELS, EROWS, COLS), F32),
                vmem((4 * ROWS, LEVELS * COLS), F32),
                vmem((2, NR, ECOLS, 128), F32),
                vmem((2, CHUNKS, NR, ECOLS, 128), F32),
                vmem((NR, ECOLS, 128), F32),
                vmem((2, 9, 8, 128), F32),
                vmem((n_gx, 1, COLS), F32),
                vmem((n_gy, 1, COLS), F32),
                dma((CHUNKS + 4,)),
                dma((CHUNKS, 4)),
                dma((CHUNKS, 4)),
                dma((4,)),
                dma((4,)),
                dma((2, 8)),
                dma((2, 8)),
                dma((n_gx,)),
                dma((n_gx,)),
                dma((n_gy,)),
                dma((n_gy,)),
            ],
            compiler_params=pltpu.CompilerParams(
                collective_id=0, has_side_effects=True, vmem_limit_bytes=28 * 1024 * 1024
            ),
        )(
            *[
                pltpu.with_memory_space_constraint(x, pltpu.HBM)
                for x in (ensemble.reshape(fields, ROWS, COLS), obs_cell, obs_level, innovation, obs_weight)
            ]
        )
        control, increment = pl.pallas_call(
            combine,
            name="combine",
            out_shape=(
                jax.ShapeDtypeStruct((fields, ROWS, COLS), F32),
                jax.ShapeDtypeStruct((LEVELS, ROWS, COLS), F32),
            ),
            in_specs=[pl.BlockSpec(memory_space=vmem)] * 4,
            out_specs=(pl.BlockSpec(memory_space=pltpu.HBM),) * 2,
            scratch_shapes=[
                vmem((fields, ROWS, COLS), F32),
                vmem((LEVELS, ROWS, COLS), F32),
                dma((BATCHES + 1,)),
            ],
            compiler_params=pltpu.CompilerParams(vmem_limit_bytes=12 * 1024 * 1024),
        )(base, grown, image, coef)
        return control.reshape(MEMBERS, LEVELS, ROWS, COLS), increment

    return jax.shard_map(
        on_device,
        mesh=mesh,
        in_specs=(P(None, None, "gy", "gx"),) + (P("gy", "gx", None),) * 4,
        out_specs=(P(None, None, "gy", "gx"), P(None, "gy", "gx")),
        check_vma=False,
    )
```
